32 devices in a mesh: row: 4 (over x, core), col: 8 (over z, y).
Axes of the slice: x: 2, y: 2, z: 4, core: 2. Of those that a mesh axis runs over, the one named last changes fastest.
Arguments:
- matrix: float32 [2048, 8192], P('col', 'row'), may hold values from -6 to 6
- basis: float32 [8192, 512], P(('row', 'col')), may hold values from -0.0625 to 0.0625
Outputs:
- root: float32 [512, 512], P('row', 'col')
- right: float32 [2048, 512], P('col')
The draws below stay inside these ranges and needn't reach their ends.
All inputs are finite; a program needn't handle non-finite values.
Results may differ from the reference program's by a relative error of at most 0.00018.
Values sent between devices are 32-bit elements; how exact they have to be, the bound alone decides.
A program may use at most 64 MiB of HBM per device.

```python
import jax
import jax.numpy as jnp
from jax import lax

N = 2048
K = 512
ITERS = 8
M = 8192


def steps_of(own_key, extent, split, smallest, largest):
    def one(axis_at, shards_of):
        draws = jax.random.uniform(jax.random.fold_in(jax.random.fold_in(own_key, 6), axis_at), (shards_of,), jnp.float32, smallest / len(split), largest / len(split))
        return jnp.repeat(jnp.exp(draws), extent[axis_at] // shards_of).reshape((-1,) + (1,) * (len(extent) - axis_at - 1))

    gain = one(*split[0])
    for cut in split[1:]:
        gain = gain * one(*cut)
    return gain


def noise(stream_key, dims, width, bound, cuts=(), kind=jnp.bfloat16):
    level = steps_of(stream_key, dims, cuts, -0.22, 0.18) if cuts else 1.0
    drawn = jax.random.normal(stream_key, dims, jnp.float32) * width * level
    return jnp.minimum(jnp.maximum(drawn, -bound), bound).astype(kind)


def setup_inputs(seed: int = 0) -> dict:
    seeds = jax.random.split(jax.random.key(seed), 3)
    matrix = noise(seeds[0], (N, M), 1.0, 6.0, ((0, 8), (1, 4)), jnp.float32)
    basis = noise(seeds[1], (M, K), M ** -0.5, 0.0625, ((0, 32),), jnp.float32)
    return dict(matrix=matrix, basis=basis)


def reference(matrix, basis):
    highest = lax.Precision.HIGHEST
    proj = lax.dot_general(basis, matrix, (((0,), (1,)), ((), ())), precision=highest)
    gram = jnp.dot(proj, proj.T, precision=highest)
    scale = jnp.sqrt(jnp.sum(gram * gram) + 1e-06)
    ident = jnp.eye(K, dtype=jnp.float32)
    upper = gram / scale
    lower = ident
    for step in range(ITERS):
        middle = 0.5 * (3.0 * ident - jnp.dot(lower, upper, precision=highest))
        upper = jnp.dot(upper, middle, precision=highest)
        lower = jnp.dot(middle, lower, precision=highest)
    root_scale = jnp.sqrt(scale)
    root = upper * root_scale
    right = jnp.dot(proj.T, lower, precision=highest) / root_scale
    return (root, right)
```

```python
import functools

import jax
import jax.numpy as jnp
from jax import lax
from jax.experimental import pallas as pl
from jax.experimental.pallas import tpu as pltpu
from jax.sharding import PartitionSpec as P

ITERS = 8
OUTER = 4
LANES = 128
VMEM = 63 * 1024 * 1024
MESH = pl.DeviceIdType.MESH


def split(x):
    hi = x.astype(jnp.bfloat16)
    lo = (x - hi.astype(jnp.float32)).astype(jnp.bfloat16)
    return hi, lo


def dot3(a, b, dims=(((1,), (0,)), ((), ()))):
    dot = functools.partial(lax.dot_general, dimension_numbers=dims, preferred_element_type=jnp.float32)
    return dot(a[0], b[0]) + dot(a[0], b[1]) + dot(a[1], b[0])


def kernel(
    nrow, ncol, size, matrix, basis, root, right,
    slab, base, blocks, pieces, ahi, alo, total, halves, parts, plane, phi, plo, shares, gram, work,
    basis_send, basis_recv, piece_send, piece_recv, half_send, half_recv, part_send, part_recv,
    away_send, away_recv, mate_send, mate_recv, share_send, share_recv,
    gram_send, gram_recv, twin_send, twin_recv, load,
):
    inner = ncol // OUTER
    nchip = nrow // 2 * inner
    row, col = lax.axis_index("row"), lax.axis_index("col")
    out, inn = col // inner, lax.rem(col, inner)
    core = lax.rem(row, 2)
    chip = row // 2 * inner + inn
    me = core * nchip + chip
    cols, depth, width = matrix.shape[0], basis.shape[0], basis.shape[1]
    tall = plane.shape[0]
    high = tall // (2 * nchip)
    chunks = width // size
    thin = size // (2 * nchip)
    mate = {"row": row + 1 - 2 * core, "col": col}

    def chip_at(k):
        return lax.rem(chip + k, nchip)

    def from_chip(k):
        return lax.rem(chip + nchip - k, nchip)

    def chip_peer(k):
        other = chip_at(k)
        return {"row": other // inner * 2 + core, "col": out * inner + lax.rem(other, inner)}

    def line_peer(k):
        return {"row": row, "col": lax.rem(out + k, OUTER) * inner + inn}

    def remote(src, dst, send, recv, device):
        return pltpu.make_async_remote_copy(
            src_ref=src, dst_ref=dst, send_sem=send, recv_sem=recv, device_id=device, device_id_type=MESH
        )

    def lanes(c):
        return pl.ds(c * size, size)

    def own_columns(at):
        return pl.ds(pl.multiple_of((at * inner + inn) * depth, depth), depth)

    loads = [pltpu.make_async_copy(basis, base, load.at[OUTER])]
    loads += [pltpu.make_async_copy(matrix.at[:, own_columns(at)], slab.at[at], load.at[at]) for at in range(OUTER)]
    for copy in loads:
        copy.start()
    barrier = pltpu.get_barrier_semaphore()
    greeted = [mate] + [chip_peer(k) for k in range(1, nchip)] + [line_peer(k) for k in range(1, OUTER)]
    for device in greeted:
        pl.semaphore_signal(barrier, inc=1, device_id=device, device_id_type=MESH)
    pl.semaphore_wait(barrier, len(greeted))

    def block_copy(source, step, c, own=False):
        here = blocks.at[source, :, lanes(c)]
        return remote(
            basis.at[:, lanes(c)] if own else here, here,
            basis_send.at[source, 0 if step > 0 else 1, c], basis_recv.at[source, c],
            {"row": row, "col": (out + step) * inner + inn},
        )

    def both_ways(step):
        return out < OUTER - 1 if step > 0 else out > 0

    def inside(source):
        return (source >= 0) & (source < OUTER)

    for step in (1, -1):
        @pl.when(both_ways(step))
        def _(step=step):
            for c in range(chunks):
                block_copy(out, step, c, True).start()

    def piece_copy(k, at):
        other = lax.rem(inn + k, inner)
        device = {"row": row, "col": out * inner + other}
        start = pl.multiple_of((at * inner + other) * depth, depth)
        return remote(
            matrix.at[:, pl.ds(start, depth)], pieces.at[k - 1, at],
            piece_send.at[k - 1, at], piece_recv.at[k - 1, at], device,
        )

    for d in range(OUTER):
        for k in range(1, inner):
            piece_copy(k, lax.rem(out + d, OUTER)).start()

    def prepare(at, k):
        if k:
            piece_copy(k, at).wait_recv()
        home = pl.ds(pl.multiple_of(lax.rem(inn + inner - k, inner) * cols, cols), cols)
        ahi[at, home, :], alo[at, home, :] = split(pieces[k - 1, at] if k else slab[at])

    def add_block(at, block, where=slice(None), first=False):
        got = dot3((ahi[at], alo[at]), split(block[:, where]))
        total[:, where] = got if first else total[:, where] + got

    def pass_on(d, c):
        for step in (1, -1):
            source = out - step * d

            @pl.when(inside(source))
            def _(source=source, step=step):
                block_copy(source, step, c).wait_recv()

                @pl.when(both_ways(step))
                def _():
                    block_copy(source, step, c).start()

    for copy in loads:
        copy.wait()
    for at in range(OUTER):
        prepare(at, 0)
    for c in range(chunks):
        pass_on(1, c)
    for k in range(1, inner):
        prepare(out, k)
    add_block(out, base, first=True)
    for d in range(2, OUTER - 1):
        for c in range(chunks):
            pass_on(d, c)
    for d in range(1, OUTER):
        for k in range(1, inner):
            prepare(lax.rem(out + d, OUTER), k)
    for d in range(1, OUTER - 1):
        for step in (1, -1):
            source = out - step * d

            @pl.when(inside(source))
            def _(source=source):
                add_block(source, blocks.at[source])

    def half(which):
        return pl.ds(pl.multiple_of(which * nchip * high, nchip * high), nchip * high)

    def part(which, at):
        return pl.ds(pl.multiple_of((which * nchip + at) * high, high), high)

    def half_copy(c):
        return remote(total.at[half(1 - core), lanes(c)], halves.at[c], half_send.at[c], half_recv.at[c], mate)

    def part_copy(c, k):
        return remote(
            total.at[part(core, chip_at(k)), lanes(c)], parts.at[c, k - 1],
            part_send.at[c, k - 1], part_recv.at[c, k - 1], chip_peer(k),
        )

    def gather(spot_of, send, recv, pair_send, pair_recv):
        def copy(which, at, c, send_sem, recv_sem, device):
            spot = spot_of(which, at, c)
            return remote(spot, spot, send_sem, recv_sem, device)

        def away(c, k, at):
            return copy(core, at, c, send.at[c, k - 1], recv.at[c, k - 1], chip_peer(k))

        def across(c, k, which):
            return copy(which, from_chip(k), c, pair_send.at[c, k], pair_recv.at[c, k], mate)

        def begin(c):
            for k in range(1, nchip):
                away(c, k, chip).start()
            across(c, 0, core).start()

        def relay(c):
            for k in range(1, nchip):
                away(c, k, from_chip(k)).wait_recv()
                across(c, k, core).start()

        def end(c):
            for k in range(nchip):
                across(c, k, 1 - core).wait_recv()

        def finish(c):
            for k in range(1, nchip):
                away(c, k, chip).wait_send()
            for k in range(nchip):
                across(c, k, core).wait_send()

        return begin, relay, end, finish

    def slim(which, at, c):
        return pl.ds(pl.multiple_of(c * size + (which * nchip + at) * thin, thin), thin)

    proj_begin, proj_relay, proj_end, proj_finish = gather(
        lambda which, at, c: plane.at[part(which, at), lanes(c)], away_send, away_recv, mate_send, mate_recv
    )
    gram_begin, gram_relay, gram_end, gram_finish = gather(
        lambda which, at, c: gram.at[slim(which, at, c), pl.ds(0, (c + 1) * size)],
        gram_send, gram_recv, twin_send, twin_recv,
    )

    def share_copy(c, k, source):
        spot = shares.at[c, source, :, pl.ds(0, (c + 1) * size)]
        return remote(spot, spot, share_send.at[c, k - 1], share_recv.at[c, k - 1], line_peer(k))

    def last_block(c):
        for d in range(OUTER - 1, OUTER):
            pass_on(d, c)
            for step in (1, -1):
                source = out - step * d

                @pl.when(inside(source))
                def _(source=source):
                    add_block(source, blocks.at[source], lanes(c))
        half_copy(c).start()

    def send_parts(c):
        half_copy(c).wait_recv()
        total[half(core), lanes(c)] = total[half(core), lanes(c)] + halves[c]
        for k in range(1, nchip):
            part_copy(c, k).start()

    def sum_parts(c):
        mine = total[part(core, chip), lanes(c)]
        for k in range(1, nchip):
            part_copy(c, k).wait_recv()
            mine = mine + parts[c, k - 1]
        plane[part(core, chip), lanes(c)] = mine
        proj_begin(c)

    def send_gram(c):
        proj_end(c)
        upto = (c + 1) * size
        phi[:, lanes(c)], plo[:, lanes(c)] = split(plane[:, lanes(c)])
        some = phi[:, lanes(c)], plo[:, lanes(c)]
        work[0:size, 0:upto] = dot3(some, (phi[:, 0:upto], plo[:, 0:upto]), (((0,), (0,)), ((), ())))
        shares[c, out, :, 0:upto] = work[pl.ds(pl.multiple_of(me * thin, thin), thin), 0:upto]
        for k in range(1, OUTER):
            share_copy(c, k, out).start()

    def sum_gram(c):
        upto = (c + 1) * size
        for k in range(1, OUTER):
            share_copy(c, k, lax.rem(out + OUTER - k, OUTER)).wait_recv()
        mine = shares[c, 0, :, 0:upto]
        for k in range(1, OUTER):
            mine = mine + shares[c, k, :, 0:upto]
        gram[slim(core, chip, c), 0:upto] = mine
        gram_begin(c)

    def mirror(c):
        gram_end(c)
        for b in range(c):
            gram[b * size : (b + 1) * size, lanes(c)] = gram[lanes(c), b * size : (b + 1) * size].T

    stages = [
        (0.0, last_block), (1.1, send_parts), (4.9, sum_parts), (8.7, proj_relay), (9.7, send_gram),
        (15.6, sum_gram), (19.4, gram_relay), (20.4, mirror),
    ]
    steps = [(2.8 * c + at, c, stage) for c in range(chunks) for at, stage in stages]
    for _, c, stage in sorted(steps, key=lambda step: step[:2]):
        stage(c)

    whole = gram[...]
    scale = jnp.sqrt(jnp.sum(whole * whole, keepdims=True) + 1e-06)
    ident = (
        lax.broadcasted_iota(jnp.int32, (width, width), 0) == lax.broadcasted_iota(jnp.int32, (width, width), 1)
    ).astype(jnp.float32)
    root_scale = jnp.sqrt(scale)
    rows = root.shape[0]
    work[0:width, :] = whole / scale
    work[width : width + cols, :] = plane[pl.ds(pl.multiple_of(inn * cols, cols), cols), :]
    work[width + cols :, :] = gram[pl.ds(pl.multiple_of(col * rows, rows), rows), :] / scale

    def polar(step, carry):
        middle = split(1.5 * ident - 0.5 * work[0:width, :])
        got = dot3(split(work[...]), middle)
        work[width:, :] = got[width:, :]
        work[0:width, :] = dot3(split(got[:width, :]), middle)
        return carry

    lax.fori_loop(0, ITERS - 1, polar, 0)
    middle = split(1.5 * ident - 0.5 * work[0:width, :])
    got = dot3(split(work[width:, :]), middle)
    right[...] = got[:cols, :] / root_scale
    root[...] = got[cols:, :] * root_scale

    for step in (1, -1):
        @pl.when(both_ways(step))
        def _(step=step):
            for c in range(chunks):
                block_copy(out, step, c, True).wait_send()
    for d in range(1, OUTER):
        for step in (1, -1):
            source = out - step * d

            @pl.when(inside(source) & both_ways(step))
            def _(source=source, step=step):
                for c in range(chunks):
                    block_copy(source, step, c).wait_send()
    for d in range(OUTER):
        for k in range(1, inner):
            piece_copy(k, lax.rem(out + d, OUTER)).wait_send()
    for c in range(chunks):
        half_copy(c).wait_send()
        for k in range(1, nchip):
            part_copy(c, k).wait_send()
        for k in range(1, OUTER):
            share_copy(c, k, out).wait_send()
        proj_finish(c)
        gram_finish(c)


def solution(mesh):
    nrow, ncol = mesh.shape["row"], mesh.shape["col"]
    inner = ncol // OUTER
    nchip = nrow // 2 * inner

    def local(matrix, basis):
        cols, (depth, width) = matrix.shape[0], basis.shape
        tall = inner * cols
        size = width if LANES % (16 * nchip) else LANES
        chunks = width // size
        vmem = pl.BlockSpec(memory_space=pltpu.VMEM)

        def array(*shape, dtype=jnp.float32):
            return pltpu.VMEM(shape, dtype)

        def pair(*shape):
            return [pltpu.SemaphoreType.DMA(shape)] * 2

        root, right = pl.pallas_call(
            functools.partial(kernel, nrow, ncol, size),
            out_shape=(
                jax.ShapeDtypeStruct((width // ncol, width), jnp.float32),
                jax.ShapeDtypeStruct((cols, width), jnp.float32),
            ),
            in_specs=[pl.BlockSpec(memory_space=pltpu.HBM)] * 2,
            out_specs=(vmem, vmem),
            scratch_shapes=[
                array(OUTER, cols, depth),
                array(depth, width),
                array(OUTER, depth, width),
                array(inner - 1, OUTER, cols, depth),
                array(OUTER, tall, depth, dtype=jnp.bfloat16),
                array(OUTER, tall, depth, dtype=jnp.bfloat16),
                array(tall, width),
                array(chunks, tall // 2, size),
                array(chunks, nchip - 1, tall // (2 * nchip), size),
                array(tall, width),
                array(tall, width, dtype=jnp.bfloat16),
                array(tall, width, dtype=jnp.bfloat16),
                array(chunks, OUTER, size // (2 * nchip), width),
                array(width, width),
                array(width + cols + width // ncol, width),
                pltpu.SemaphoreType.DMA((OUTER, 2, chunks)),
                pltpu.SemaphoreType.DMA((OUTER, chunks)),
                *pair(inner - 1, OUTER),
                *pair(chunks),
                *pair(chunks, nchip - 1),
                *pair(chunks, nchip - 1),
                *pair(chunks, nchip),
                *pair(chunks, OUTER - 1),
                *pair(chunks, nchip - 1),
                *pair(chunks, nchip),
                pltpu.SemaphoreType.DMA((OUTER + 1,)),
            ],
            compiler_params=pltpu.CompilerParams(
                collective_id=0, has_side_effects=True, vmem_limit_bytes=VMEM
            ),
        )(matrix, basis)
        long = width // nrow
        part = lax.dynamic_slice(root, (0, lax.axis_index("row") * long), (width // ncol, long))
        return part.T, right

    return jax.shard_map(
        local,
        mesh=mesh,
        in_specs=(P("col", "row"), P(("row", "col"), None)),
        out_specs=(P("row", "col"), P("col", None)),
        check_vma=False,
    )
```

```python
import functools

import jax
import jax.numpy as jnp
from jax import lax
from jax.experimental import pallas as pl
from jax.experimental.pallas import tpu as pltpu
from jax.sharding import PartitionSpec as P

ITERS = 8
OUTER = 4
LANES = 128
VMEM = 62 * 1024 * 1024
MESH = pl.DeviceIdType.MESH


def split(x):
    hi = x.astype(jnp.bfloat16)
    lo = (x - hi.astype(jnp.float32)).astype(jnp.bfloat16)
    return hi, lo


def dot(a, b, dims=(((1,), (0,)), ((), ()))):
    return lax.dot_general(a, b, dimension_numbers=dims, preferred_element_type=jnp.float32)


def dot3(a, b, dims=(((1,), (0,)), ((), ()))):
    return dot(a[0], b[0], dims) + dot(a[0], b[1], dims) + dot(a[1], b[0], dims)


def kernel(
    nrow, ncol, size, matrix, basis, root, right,
    slab, base, blocks, pieces, ahi, alo, total, halves, parts, plane, phi, plo, shares, gram, work,
    basis_send, basis_recv, piece_send, piece_recv, half_send, half_recv, part_send, part_recv,
    away_send, away_recv, mate_send, mate_recv, share_send, share_recv,
    gram_send, gram_recv, twin_send, twin_recv, load,
):
    inner = ncol // OUTER
    nchip = nrow // 2 * inner
    row, col = lax.axis_index("row"), lax.axis_index("col")
    out, inn = col // inner, lax.rem(col, inner)
    core = lax.rem(row, 2)
    chip = row // 2 * inner + inn
    me = core * nchip + chip
    cols, depth, width = matrix.shape[0], basis.shape[0], basis.shape[1]
    tall = plane.shape[0]
    high = tall // (2 * nchip)
    chunks = width // size
    thin = size // (2 * nchip)
    mate = {"row": row + 1 - 2 * core, "col": col}

    def chip_at(k):
        return lax.rem(chip + k, nchip)

    def from_chip(k):
        return lax.rem(chip + nchip - k, nchip)

    def chip_peer(k):
        other = chip_at(k)
        return {"row": other // inner * 2 + core, "col": out * inner + lax.rem(other, inner)}

    def line_peer(k):
        return {"row": row, "col": lax.rem(out + k, OUTER) * inner + inn}

    def remote(src, dst, send, recv, device):
        return pltpu.make_async_remote_copy(
            src_ref=src, dst_ref=dst, send_sem=send, recv_sem=recv, device_id=device, device_id_type=MESH
        )

    def lanes(c):
        return pl.ds(c * size, size)

    def own_columns(at):
        return pl.ds(pl.multiple_of((at * inner + inn) * depth, depth), depth)

    loads = [pltpu.make_async_copy(basis, base, load.at[OUTER])]
    loads += [pltpu.make_async_copy(matrix.at[:, own_columns(at)], slab.at[at], load.at[at]) for at in range(OUTER)]
    for copy in loads:
        copy.start()
    barrier = pltpu.get_barrier_semaphore()
    greeted = [mate] + [chip_peer(k) for k in range(1, nchip)] + [line_peer(k) for k in range(1, OUTER)]
    for device in greeted:
        pl.semaphore_signal(barrier, inc=1, device_id=device, device_id_type=MESH)
    pl.semaphore_wait(barrier, len(greeted))

    def block_copy(source, step, c, own=False):
        here = blocks.at[source, :, lanes(c)]
        return remote(
            basis.at[:, lanes(c)] if own else here, here,
            basis_send.at[source, 0 if step > 0 else 1, c], basis_recv.at[source, c],
            {"row": row, "col": (out + step) * inner + inn},
        )

    def both_ways(step):
        return out < OUTER - 1 if step > 0 else out > 0

    def inside(source):
        return (source >= 0) & (source < OUTER)

    for step in (1, -1):
        @pl.when(both_ways(step))
        def _(step=step):
            for c in range(chunks):
                block_copy(out, step, c, True).start()

    def piece_copy(k, at):
        other = lax.rem(inn + k, inner)
        device = {"row": row, "col": out * inner + other}
        start = pl.multiple_of((at * inner + other) * depth, depth)
        return remote(
            matrix.at[:, pl.ds(start, depth)], pieces.at[k - 1, at],
            piece_send.at[k - 1, at], piece_recv.at[k - 1, at], device,
        )

    for d in range(OUTER):
        for k in range(1, inner):
            piece_copy(k, lax.rem(out + d, OUTER)).start()

    def prepare(at, k):
        if k:
            piece_copy(k, at).wait_recv()
        home = pl.ds(pl.multiple_of(lax.rem(inn + inner - k, inner) * cols, cols), cols)
        ahi[at, home, :], alo[at, home, :] = split(pieces[k - 1, at] if k else slab[at])

    def add_block(at, block, where=slice(None), first=False):
        got = dot3((ahi[at], alo[at]), split(block[:, where]))
        total[:, where] = got if first else total[:, where] + got

    def pass_on(d, c):
        for step in (1, -1):
            source = out - step * d

            @pl.when(inside(source))
            def _(source=source, step=step):
                block_copy(source, step, c).wait_recv()

                @pl.when(both_ways(step))
                def _():
                    block_copy(source, step, c).start()

    for copy in loads:
        copy.wait()
    for at in range(OUTER):
        prepare(at, 0)
    for c in range(chunks):
        pass_on(1, c)
    for k in range(1, inner):
        prepare(out, k)
    add_block(out, base, first=True)
    for d in range(2, OUTER - 1):
        for c in range(chunks):
            pass_on(d, c)
    for d in range(1, OUTER):
        for k in range(1, inner):
            prepare(lax.rem(out + d, OUTER), k)
    for d in range(1, OUTER - 1):
        for step in (1, -1):
            source = out - step * d

            @pl.when(inside(source))
            def _(source=source):
                add_block(source, blocks.at[source])

    def half(which):
        return pl.ds(pl.multiple_of(which * nchip * high, nchip * high), nchip * high)

    def part(which, at):
        return pl.ds(pl.multiple_of((which * nchip + at) * high, high), high)

    def half_copy(c):
        return remote(total.at[half(1 - core), lanes(c)], halves.at[c], half_send.at[c], half_recv.at[c], mate)

    def part_copy(c, k):
        return remote(
            total.at[part(core, chip_at(k)), lanes(c)], parts.at[c, k - 1],
            part_send.at[c, k - 1], part_recv.at[c, k - 1], chip_peer(k),
        )

    def gather(spot_of, send, recv, pair_send, pair_recv):
        def copy(which, at, c, send_sem, recv_sem, device):
            spot = spot_of(which, at, c)
            return remote(spot, spot, send_sem, recv_sem, device)

        def away(c, k, at):
            return copy(core, at, c, send.at[c, k - 1], recv.at[c, k - 1], chip_peer(k))

        def across(c, k, which):
            return copy(which, from_chip(k), c, pair_send.at[c, k], pair_recv.at[c, k], mate)

        def begin(c):
            for k in range(1, nchip):
                away(c, k, chip).start()
            across(c, 0, core).start()

        def relay(c):
            for k in range(1, nchip):
                away(c, k, from_chip(k)).wait_recv()
                across(c, k, core).start()

        def end(c):
            for k in range(nchip):
                across(c, k, 1 - core).wait_recv()

        def finish(c):
            for k in range(1, nchip):
                away(c, k, chip).wait_send()
            for k in range(nchip):
                across(c, k, core).wait_send()

        return begin, relay, end, finish

    def slim(which, at, c):
        return pl.ds(pl.multiple_of(c * size + (which * nchip + at) * thin, thin), thin)

    proj_begin, proj_relay, proj_end, proj_finish = gather(
        lambda which, at, c: plane.at[part(which, at), lanes(c)], away_send, away_recv, mate_send, mate_recv
    )
    gram_begin, gram_relay, gram_end, gram_finish = gather(
        lambda which, at, c: gram.at[slim(which, at, c), pl.ds(0, (c + 1) * size)],
        gram_send, gram_recv, twin_send, twin_recv,
    )

    def share_copy(c, k, source):
        spot = shares.at[c, source, :, pl.ds(0, (c + 1) * size)]
        return remote(spot, spot, share_send.at[c, k - 1], share_recv.at[c, k - 1], line_peer(k))

    def last_block(c):
        for d in range(OUTER - 1, OUTER):
            pass_on(d, c)
            for step in (1, -1):
                source = out - step * d

                @pl.when(inside(source))
                def _(source=source):
                    add_block(source, blocks.at[source], lanes(c))
        half_copy(c).start()

    def send_parts(c):
        half_copy(c).wait_recv()
        total[half(core), lanes(c)] = total[half(core), lanes(c)] + halves[c]
        for k in range(1, nchip):
            part_copy(c, k).start()

    def sum_parts(c):
        mine = total[part(core, chip), lanes(c)]
        for k in range(1, nchip):
            part_copy(c, k).wait_recv()
            mine = mine + parts[c, k - 1]
        plane[part(core, chip), lanes(c)] = mine
        proj_begin(c)

    def send_gram(c):
        proj_end(c)
        upto = (c + 1) * size
        phi[:, lanes(c)], plo[:, lanes(c)] = split(plane[:, lanes(c)])
        some = phi[:, lanes(c)], plo[:, lanes(c)]
        work[0:size, 0:upto] = dot3(some, (phi[:, 0:upto], plo[:, 0:upto]), (((0,), (0,)), ((), ())))
        shares[c, out, :, 0:upto] = work[pl.ds(pl.multiple_of(me * thin, thin), thin), 0:upto]
        for k in range(1, OUTER):
            share_copy(c, k, out).start()

    def sum_gram(c):
        upto = (c + 1) * size
        for k in range(1, OUTER):
            share_copy(c, k, lax.rem(out + OUTER - k, OUTER)).wait_recv()
        mine = shares[c, 0, :, 0:upto]
        for k in range(1, OUTER):
            mine = mine + shares[c, k, :, 0:upto]
        gram[slim(core, chip, c), 0:upto] = mine
        gram_begin(c)

    def mirror(c):
        gram_end(c)
        for b in range(c):
            gram[b * size : (b + 1) * size, lanes(c)] = gram[lanes(c), b * size : (b + 1) * size].T

    stages = [
        (0.0, last_block), (1.1, send_parts), (4.9, sum_parts), (8.7, proj_relay), (9.7, send_gram),
        (15.6, sum_gram), (19.4, gram_relay), (20.4, mirror),
    ]
    steps = [(2.8 * c + at, c, stage) for c in range(chunks) for at, stage in stages]
    for _, c, stage in sorted(steps, key=lambda step: step[:2]):
        stage(c)

    whole = gram[...]
    scale = jnp.sqrt(jnp.sum(whole * whole, keepdims=True) + 1e-06)
    root_scale = jnp.sqrt(scale)
    rows = root.shape[0]
    work[0:width, :] = whole / scale
    for c in range(chunks):
        square = gram[lanes(c), lanes(c)]
        work[lanes(c), lanes(c)] = 0.5 * (square + square.T) / scale
    work[width : width + cols, :] = plane[pl.ds(pl.multiple_of(inn * cols, cols), cols), :]
    work[width + cols :, :] = gram[pl.ds(pl.multiple_of(col * rows, rows), rows), :] / scale

    def halves_squared(x):
        half_product = dot(x[0], 0.5 * x[0]) + dot(x[0], x[1])
        return half_product + half_product.T

    def factor(w, w_halves):
        e = halves_squared(w_halves) - 4.5 * w
        return 0.0625 * halves_squared(split(e)) + (0.421875 * e - 0.5390625 * w)

    for step in range(ITERS // 2):
        w = work[0:width, :]
        w_halves = split(w)
        f = factor(w, w_halves)
        f_halves = split(f)
        rest = work[width:, :]
        if step == ITERS // 2 - 1:
            got = 2.25 * rest + dot3(split(rest), f_halves)
            right[...] = got[:cols, :] / root_scale
            root[...] = got[cols:, :] * root_scale
        else:
            growth = halves_squared(f_halves) + 4.5 * f
            work[width:, :] = 2.25 * rest + dot3(split(rest), f_halves)
            product = dot3(w_halves, split(growth))
            work[0:width, :] = 5.0625 * w + 0.5 * (product + product.T)

    for step in (1, -1):
        @pl.when(both_ways(step))
        def _(step=step):
            for c in range(chunks):
                block_copy(out, step, c, True).wait_send()
    for d in range(1, OUTER):
        for step in (1, -1):
            source = out - step * d

            @pl.when(inside(source) & both_ways(step))
            def _(source=source, step=step):
                for c in range(chunks):
                    block_copy(source, step, c).wait_send()
    for d in range(OUTER):
        for k in range(1, inner):
            piece_copy(k, lax.rem(out + d, OUTER)).wait_send()
    for c in range(chunks):
        half_copy(c).wait_send()
        for k in range(1, nchip):
            part_copy(c, k).wait_send()
        for k in range(1, OUTER):
            share_copy(c, k, out).wait_send()
        proj_finish(c)
        gram_finish(c)


def solution(mesh):
    nrow, ncol = mesh.shape["row"], mesh.shape["col"]
    inner = ncol // OUTER
    nchip = nrow // 2 * inner

    def local(matrix, basis):
        cols, (depth, width) = matrix.shape[0], basis.shape
        tall = inner * cols
        size = width if LANES % (16 * nchip) else LANES
        chunks = width // size
        vmem = pl.BlockSpec(memory_space=pltpu.VMEM)

        def array(*shape, dtype=jnp.float32):
            return pltpu.VMEM(shape, dtype)

        def pair(*shape):
            return [pltpu.SemaphoreType.DMA(shape)] * 2

        root, right = pl.pallas_call(
            functools.partial(kernel, nrow, ncol, size),
            out_shape=(
                array(width // ncol, width),
                array(cols, width),
            ),
            in_specs=[pl.BlockSpec(memory_space=pltpu.HBM)] * 2,
            out_specs=(vmem, vmem),
            scratch_shapes=[
                array(OUTER, cols, depth),
                array(depth, width),
                array(OUTER, depth, width),
                array(inner - 1, OUTER, cols, depth),
                array(OUTER, tall, depth, dtype=jnp.bfloat16),
                array(OUTER, tall, depth, dtype=jnp.bfloat16),
                array(tall, width),
                array(chunks, tall // 2, size),
                array(chunks, nchip - 1, tall // (2 * nchip), size),
                array(tall, width),
                array(tall, width, dtype=jnp.bfloat16),
                array(tall, width, dtype=jnp.bfloat16),
                array(chunks, OUTER, size // (2 * nchip), width),
                array(width, width),
                array(width + cols + width // ncol, width),
                pltpu.SemaphoreType.DMA((OUTER, 2, chunks)),
                pltpu.SemaphoreType.DMA((OUTER, chunks)),
                *pair(inner - 1, OUTER),
                *pair(chunks),
                *pair(chunks, nchip - 1),
                *pair(chunks, nchip - 1),
                *pair(chunks, nchip),
                *pair(chunks, OUTER - 1),
                *pair(chunks, nchip - 1),
                *pair(chunks, nchip),
                pltpu.SemaphoreType.DMA((OUTER + 1,)),
            ],
            compiler_params=pltpu.CompilerParams(
                collective_id=0, has_side_effects=True, vmem_limit_bytes=VMEM
            ),
        )(matrix, basis)
        long = width // nrow
        part = lax.dynamic_slice(root, (0, lax.axis_index("row") * long), (width // ncol, long))
        return part.T, right

    return jax.shard_map(
        local,
        mesh=mesh,
        in_specs=(P("col", "row"), P(("row", "col"), None)),
        out_specs=(P("row", "col"), P("col", None)),
        check_vma=False,
    )
```

```python
import functools

import jax
import jax.numpy as jnp
from jax import lax
from jax.experimental import pallas as pl
from jax.experimental.pallas import tpu as pltpu
from jax.sharding import PartitionSpec as P

ITERS = 8
OUTER = 4
LANES = 128
VMEM = 62 * 1024 * 1024
MESH = pl.DeviceIdType.MESH


def split(x):
    hi = x.astype(jnp.bfloat16)
    lo = (x - hi.astype(jnp.float32)).astype(jnp.bfloat16)
    return hi, lo


def dot(a, b, dims=(((1,), (0,)), ((), ()))):
    return lax.dot_general(a, b, dimension_numbers=dims, preferred_element_type=jnp.float32)


def dot3(a, b, dims=(((1,), (0,)), ((), ()))):
    return dot(a[0], b[0], dims) + dot(a[0], b[1], dims) + dot(a[1], b[0], dims)


def kernel(
    nrow, ncol, size, taken, matrix, basis, root, right,
    slab, base, blocks, pieces, ahi, alo, total, halves, parts, plane, phi, plo, shares, gram, work,
    given, lent, lent_halves, lent_parts, lent_sums, gifts,
    basis_send, basis_recv, piece_send, piece_recv, half_send, half_recv, part_send, part_recv,
    away_send, away_recv, mate_send, mate_recv, share_send, share_recv,
    gram_send, gram_recv, twin_send, twin_recv, load,
    given_send, given_recv, lent_half_send, lent_half_recv, lent_part_send, lent_part_recv, gift_send, gift_recv,
):
    inner = ncol // OUTER
    nchip = nrow // 2 * inner
    row, col = lax.axis_index("row"), lax.axis_index("col")
    out, inn = col // inner, lax.rem(col, inner)
    core = lax.rem(row, 2)
    chip = row // 2 * inner + inn
    me = core * nchip + chip
    cols, depth, width = matrix.shape[0], basis.shape[0], basis.shape[1]
    tall = plane.shape[0]
    high = tall // (2 * nchip)
    chunks = width // size
    thin = size // (2 * nchip)
    mate = {"row": row + 1 - 2 * core, "col": col}

    def chip_at(k):
        return lax.rem(chip + k, nchip)

    def from_chip(k):
        return lax.rem(chip + nchip - k, nchip)

    def chip_peer(k):
        other = chip_at(k)
        return {"row": other // inner * 2 + core, "col": out * inner + lax.rem(other, inner)}

    def line_peer(k):
        return {"row": row, "col": lax.rem(out + k, OUTER) * inner + inn}

    def remote(src, dst, send, recv, device):
        return pltpu.make_async_remote_copy(
            src_ref=src, dst_ref=dst, send_sem=send, recv_sem=recv, device_id=device, device_id_type=MESH
        )

    aside = out + 1 - 2 * lax.rem(out, 2)
    far = OUTER - 1 - out
    is_end = (out == 0) | (out == OUTER - 1)
    is_middle = (out > 0) & (out < OUTER - 1)
    aside_peer = {"row": row, "col": aside * inner + inn}

    def lanes(c):
        return pl.ds(c * size, size)

    def own_columns(at):
        return pl.ds(pl.multiple_of((at * inner + inn) * depth, depth), depth)

    loads = [pltpu.make_async_copy(basis, base, load.at[OUTER])]
    loads += [pltpu.make_async_copy(matrix.at[:, own_columns(at)], slab.at[at], load.at[at]) for at in range(OUTER)]
    for copy in loads:
        copy.start()
    barrier = pltpu.get_barrier_semaphore()
    greeted = [mate] + [chip_peer(k) for k in range(1, nchip)] + [line_peer(k) for k in range(1, OUTER)]
    for device in greeted:
        pl.semaphore_signal(barrier, inc=1, device_id=device, device_id_type=MESH)
    pl.semaphore_wait(barrier, len(greeted))

    def block_copy(source, step, c, own=False):
        here = blocks.at[source, :, lanes(c)]
        return remote(
            basis.at[:, lanes(c)] if own else here, here,
            basis_send.at[source, 0 if step > 0 else 1, c], basis_recv.at[source, c],
            {"row": row, "col": (out + step) * inner + inn},
        )

    def both_ways(step):
        return out < OUTER - 1 if step > 0 else out > 0

    def inside(source):
        return (source >= 0) & (source < OUTER)

    for step in (1, -1):
        @pl.when(both_ways(step))
        def _(step=step):
            for c in range(chunks):
                block_copy(out, step, c, True).start()

    def piece_copy(k, at):
        other = lax.rem(inn + k, inner)
        device = {"row": row, "col": out * inner + other}
        start = pl.multiple_of((at * inner + other) * depth, depth)
        return remote(
            matrix.at[:, pl.ds(start, depth)], pieces.at[k - 1, at],
            piece_send.at[k - 1, at], piece_recv.at[k - 1, at], device,
        )

    turn = [far, out, aside, OUTER - 1 - aside]
    for at in turn:
        for k in range(1, inner):
            piece_copy(k, at).start()

    def given_copy(k):
        start = pl.multiple_of((far * inner + inn) * depth, depth)
        return remote(
            pieces.at[k - 1, far] if k else matrix.at[:, pl.ds(start, depth)], given.at[k],
            given_send.at[k], given_recv.at[k], aside_peer,
        )

    if taken:
        @pl.when(is_end)
        def _():
            given_copy(0).start()

    def home(k):
        return pl.ds(pl.multiple_of(lax.rem(inn + inner - k, inner) * cols, cols), cols)

    def prepare(at, k):
        if k:
            piece_copy(k, at).wait_recv()
        ahi[at, home(k), :], alo[at, home(k), :] = split(pieces[k - 1, at] if k else slab[at])

    def add_block(at, block, where=slice(None), first=False):
        got = dot3((ahi[at], alo[at]), split(block[:, where]))
        total[:, where] = got if first else total[:, where] + got

    def pass_on(d, c):
        goes_on = d < OUTER - 2 or c not in taken
        for step in (1, -1):
            source = out - step * d

            @pl.when(inside(source))
            def _(source=source, step=step):
                block_copy(source, step, c).wait_recv()
                if goes_on:
                    @pl.when(both_ways(step))
                    def _():
                        block_copy(source, step, c).start()

    for copy in loads:
        copy.wait()
    for at in range(OUTER):
        prepare(at, 0)

    def add_turn(at, condition):
        def add():
            add_block(at, blocks.at[at])

        if condition is None:
            add()
        else:
            pl.when(condition)(add)

    for c in range(chunks):
        pass_on(1, c)
        if c == 0:
            for k in range(1, inner):
                prepare(far, k)
            if taken:
                @pl.when(is_end)
                def _():
                    for k in range(1, inner):
                        given_copy(k).start()
    for k in range(1, inner):
        prepare(out, k)
    add_block(out, base, first=True)
    add_turn(far, is_middle)
    for c in range(chunks):
        pass_on(2, c)
        if c == chunks // 2 - 1:
            for k in range(1, inner):
                prepare(aside, k)
            add_turn(aside, None)
    if chunks == 1:
        for k in range(1, inner):
            prepare(aside, k)
        add_turn(aside, None)
    for k in range(1, inner):
        prepare(OUTER - 1 - aside, k)
    if taken:
        @pl.when(is_middle)
        def _():
            for k in range(inner):
                given_copy(k).wait_recv()
                ahi[OUTER, home(k), :], alo[OUTER, home(k), :] = split(given[k])

    def lend(n):
        block = blocks[OUTER - 1 - aside, :, lanes(taken[n])]
        lent[:, lanes(n)] = dot3((ahi[OUTER], alo[OUTER]), split(block))

    def half(which):
        return pl.ds(pl.multiple_of(which * nchip * high, nchip * high), nchip * high)

    def part(which, at):
        return pl.ds(pl.multiple_of((which * nchip + at) * high, high), high)

    def half_copy(c):
        return remote(total.at[half(1 - core), lanes(c)], halves.at[c], half_send.at[c], half_recv.at[c], mate)

    def part_copy(c, k):
        return remote(
            total.at[part(core, chip_at(k)), lanes(c)], parts.at[c, k - 1],
            part_send.at[c, k - 1], part_recv.at[c, k - 1], chip_peer(k),
        )

    def lent_half_copy(n):
        return remote(
            lent.at[half(1 - core), lanes(n)], lent_halves.at[n], lent_half_send.at[n], lent_half_recv.at[n], mate
        )

    def lent_part_copy(n, k):
        return remote(
            lent.at[part(core, chip_at(k)), lanes(n)], lent_parts.at[n, k - 1],
            lent_part_send.at[n, k - 1], lent_part_recv.at[n, k - 1], chip_peer(k),
        )

    def gift_copy(n):
        return remote(lent_sums.at[n], gifts.at[n], gift_send.at[n], gift_recv.at[n], aside_peer)

    def lend_halves(n):
        lend(n)
        lent_half_copy(n).start()

    def lend_parts(n):
        lent_half_copy(n).wait_recv()
        lent[half(core), lanes(n)] = lent[half(core), lanes(n)] + lent_halves[n]
        for k in range(1, nchip):
            lent_part_copy(n, k).start()

    def give(n):
        mine = lent[part(core, chip), lanes(n)]
        for k in range(1, nchip):
            lent_part_copy(n, k).wait_recv()
            mine = mine + lent_parts[n, k - 1]
        lent_sums[n] = mine
        gift_copy(n).start()

    def gather(spot_of, send, recv, pair_send, pair_recv):
        def copy(which, at, c, send_sem, recv_sem, device):
            spot = spot_of(which, at, c)
            return remote(spot, spot, send_sem, recv_sem, device)

        def away(c, k, at):
            return copy(core, at, c, send.at[c, k - 1], recv.at[c, k - 1], chip_peer(k))

        def across(c, k, which):
            return copy(which, from_chip(k), c, pair_send.at[c, k], pair_recv.at[c, k], mate)

        def begin(c):
            for k in range(1, nchip):
                away(c, k, chip).start()
            across(c, 0, core).start()

        def relay(c):
            for k in range(1, nchip):
                away(c, k, from_chip(k)).wait_recv()
                across(c, k, core).start()

        def end(c):
            for k in range(nchip):
                across(c, k, 1 - core).wait_recv()

        def finish(c):
            for k in range(1, nchip):
                away(c, k, chip).wait_send()
            for k in range(nchip):
                across(c, k, core).wait_send()

        return begin, relay, end, finish

    def slim(which, at, c):
        return pl.ds(pl.multiple_of(c * size + (which * nchip + at) * thin, thin), thin)

    proj_begin, proj_relay, proj_end, proj_finish = gather(
        lambda which, at, c: plane.at[part(which, at), lanes(c)], away_send, away_recv, mate_send, mate_recv
    )
    gram_begin, gram_relay, gram_end, gram_finish = gather(
        lambda which, at, c: gram.at[slim(which, at, c), pl.ds(0, (c + 1) * size)],
        gram_send, gram_recv, twin_send, twin_recv,
    )

    def share(c, slot):
        return shares.at[c, slot, :, pl.ds(0, (c + 1) * size)]

    def share_copy(c):
        return remote(share(c, 0), share(c, 1), share_send.at[c, 0], share_recv.at[c, 0], aside_peer)

    def pair_copy(c, n):
        plane_to = far if n == 0 else OUTER - 1 - aside
        device = {"row": row, "col": plane_to * inner + inn}
        return remote(share(c, 2), share(c, 3), share_send.at[c, 1 + n], share_recv.at[c, 1], device)

    def send_half(c):
        half_copy(c).start()

    def last_block(c):
        pass_on(OUTER - 1, c)
        add_block(far, blocks.at[far], lanes(c))
        send_half(c)

    def send_parts(c):
        half_copy(c).wait_recv()
        total[half(core), lanes(c)] = total[half(core), lanes(c)] + halves[c]
        for k in range(1, nchip):
            part_copy(c, k).start()

    def sum_parts(c, gift=None):
        mine = total[part(core, chip), lanes(c)]
        for k in range(1, nchip):
            part_copy(c, k).wait_recv()
            mine = mine + parts[c, k - 1]
        if gift is not None:
            gift_copy(gift).wait_recv()
            mine = mine + gifts[gift]
        plane[part(core, chip), lanes(c)] = mine
        proj_begin(c)

    def send_gram(c):
        proj_end(c)
        upto = (c + 1) * size
        phi[:, lanes(c)], plo[:, lanes(c)] = split(plane[:, lanes(c)])
        some = phi[:, lanes(c)], plo[:, lanes(c)]
        work[0:size, 0:upto] = dot3(some, (phi[:, 0:upto], plo[:, 0:upto]), (((0,), (0,)), ((), ())))
        shares[c, 0, :, 0:upto] = work[pl.ds(pl.multiple_of(me * thin, thin), thin), 0:upto]
        share_copy(c).start()

    def sum_pair(c):
        upto = (c + 1) * size
        share_copy(c).wait_recv()
        shares[c, 2, :, 0:upto] = shares[c, 0, :, 0:upto] + shares[c, 1, :, 0:upto]

    def send_pair(c):
        sum_pair(c)
        for n in range(2):
            pair_copy(c, n).start()

    def sum_gram(c):
        upto = (c + 1) * size
        pair_copy(c, 0).wait_recv()
        gram[slim(core, chip, c), 0:upto] = shares[c, 2, :, 0:upto] + shares[c, 3, :, 0:upto]
        gram_begin(c)

    def mirror(c):
        gram_end(c)
        for b in range(c):
            gram[b * size : (b + 1) * size, lanes(c)] = gram[lanes(c), b * size : (b + 1) * size].T

    def sum_with_gift(c):
        sum_parts(c, taken.index(c))

    last = OUTER - 1 - aside

    def add_last(where):
        add_block(last, blocks.at[last], where)

    if chunks == 4:
        end_order = [
            (add_last, slice(size, 3 * size)),
            (send_half, 1), (send_half, 2), (add_last, slice(0, size)), (add_last, slice(3 * size, width)),
            (send_parts, 1), (send_parts, 2), (last_block, 0), (send_parts, 0),
            (last_block, 3), (send_parts, 3), (sum_parts, 0), (sum_with_gift, 1), (sum_with_gift, 2), (sum_parts, 3),
        ]
        middle_order = [
            (add_last, slice(0, 2 * size)), (send_half, 0), (send_half, 1), (lend_halves, 0), (lend_halves, 1),
            (send_parts, 0), (add_last, slice(2 * size, width)), (send_half, 2), (send_half, 3), (lend_parts, 0), (lend_parts, 1), (send_parts, 1), (sum_parts, 0), (send_parts, 2),
            (send_parts, 3), (give, 0), (give, 1), (sum_parts, 1), (proj_relay, 0), (sum_parts, 2), (sum_parts, 3),
        ]
    else:
        lots = range(len(taken))
        each = range(chunks)
        end_order = [(add_last, slice(None))] + [(send_half if c in taken else last_block, c) for c in each]
        end_order += [(send_parts, c) for c in each]
        end_order += [(sum_with_gift if c in taken else sum_parts, c) for c in each]
        middle_order = [(add_last, slice(None))]
        middle_order += [(stage, n) for stage in (lend_halves, lend_parts, give) for n in lots]
        middle_order += [(stage, c) for stage in (send_half, send_parts, sum_parts) for c in each]

    for role, order in ((is_end, end_order), (is_middle, middle_order)):
        for c in range(chunks + 2):
            if c < chunks and (proj_relay, c) not in order:
                order.append((proj_relay, c))
            if 0 < c <= chunks:
                order.append((send_gram, c - 1))
            if c > 1 and role is is_middle:
                order.append((send_pair, c - 2))
        for c in range(chunks):
            if role is is_end:
                order.append((sum_pair, c))
            order.append((sum_gram, c))

        @pl.when(role)
        def _(order=order):
            for stage, c in order:
                stage(c)

    for c in range(chunks + 1):
        if c < chunks:
            gram_relay(c)
        if c:
            mirror(c - 1)

    whole = gram[...]
    scale = jnp.sqrt(jnp.sum(whole * whole, keepdims=True) + 1e-06)
    root_scale = jnp.sqrt(scale)
    rows = root.shape[0]
    work[0:width, :] = whole / scale
    for c in range(chunks):
        square = gram[lanes(c), lanes(c)]
        work[lanes(c), lanes(c)] = 0.5 * (square + square.T) / scale
    work[width : width + cols, :] = plane[pl.ds(pl.multiple_of(inn * cols, cols), cols), :]
    work[width + cols :, :] = gram[pl.ds(pl.multiple_of(col * rows, rows), rows), :] / scale

    def halves_squared(x):
        cross = dot(x[0], x[1]).astype(jnp.bfloat16)
        return dot(x[0], x[0]) + (cross.astype(jnp.float32) + cross.T.astype(jnp.float32))

    for step in range(ITERS // 2):
        w = work[0:width, :]
        w_halves = split(w)
        e = halves_squared(w_halves) - 4.5 * w
        f = 0.0625 * halves_squared(split(e)) + (0.421875 * e - 0.5390625 * w)
        f_halves = split(f)
        rest = work[width:, :]
        if step == ITERS // 2 - 1:
            got = 2.25 * rest + dot3(split(rest), f_halves)
            right[...] = got[:cols, :] / root_scale
            root[...] = got[cols:, :] * root_scale
            break
        growth = split(halves_squared(f_halves) + 4.5 * f)
        work[width:, :] = 2.25 * rest + dot3(split(rest), f_halves)
        for start in range(0, width, LANES):
            band, after = slice(start, start + LANES), slice(start + LANES, width)
            product = dot3([half[band] for half in w_halves], [half[:, start:] for half in growth])
            square = product[:, :LANES]
            work[band, band] = 5.0625 * w[band, band] + 0.5 * (square + square.T)
            if start + LANES < width:
                work[band, after] = 5.0625 * w[band, after] + product[:, LANES:]
                work[after, band] = work[band, after].T

    for step in (1, -1):
        @pl.when(both_ways(step))
        def _(step=step):
            for c in range(chunks):
                block_copy(out, step, c, True).wait_send()
    for d in range(1, OUTER):
        for step in (1, -1):
            source = out - step * d

            @pl.when(inside(source) & both_ways(step))
            def _(source=source, step=step, d=d):
                for c in range(chunks):
                    if d < OUTER - 2 or c not in taken:
                        block_copy(source, step, c).wait_send()
    for at in turn:
        for k in range(1, inner):
            piece_copy(k, at).wait_send()
    if taken:
        @pl.when(is_end)
        def _():
            for k in range(inner):
                given_copy(k).wait_send()

        @pl.when(is_middle)
        def _():
            for n in range(len(taken)):
                lent_half_copy(n).wait_send()
                for k in range(1, nchip):
                    lent_part_copy(n, k).wait_send()
                gift_copy(n).wait_send()

    @pl.when(is_middle)
    def _():
        for c in range(chunks):
            for n in range(2):
                pair_copy(c, n).wait_send()

    for c in range(chunks):
        half_copy(c).wait_send()
        for k in range(1, nchip):
            part_copy(c, k).wait_send()
        share_copy(c).wait_send()
        proj_finish(c)
        gram_finish(c)


def solution(mesh):
    nrow, ncol = mesh.shape["row"], mesh.shape["col"]
    inner = ncol // OUTER
    nchip = nrow // 2 * inner

    def local(matrix, basis):
        cols, (depth, width) = matrix.shape[0], basis.shape
        tall = inner * cols
        size = width if LANES % (16 * nchip) else LANES
        chunks = width // size
        taken = tuple(range(1, chunks - 1))
        lots = max(len(taken), 1)
        vmem = pl.BlockSpec(memory_space=pltpu.VMEM)

        def array(*shape, dtype=jnp.float32):
            return pltpu.VMEM(shape, dtype)

        def pair(*shape):
            return [pltpu.SemaphoreType.DMA(shape)] * 2

        root, right = pl.pallas_call(
            functools.partial(kernel, nrow, ncol, size, taken),
            out_shape=(
                array(width // ncol, width),
                array(cols, width),
            ),
            in_specs=[pl.BlockSpec(memory_space=pltpu.HBM)] * 2,
            out_specs=(vmem, vmem),
            scratch_shapes=[
                array(OUTER, cols, depth),
                array(depth, width),
                array(OUTER, depth, width),
                array(inner - 1, OUTER, cols, depth),
                array(OUTER + 1, tall, depth, dtype=jnp.bfloat16),
                array(OUTER + 1, tall, depth, dtype=jnp.bfloat16),
                array(tall, width),
                array(chunks, tall // 2, size),
                array(chunks, nchip - 1, tall // (2 * nchip), size),
                array(tall, width),
                array(tall, width, dtype=jnp.bfloat16),
                array(tall, width, dtype=jnp.bfloat16),
                array(chunks, OUTER, size // (2 * nchip), width),
                array(width, width),
                array(width + cols + width // ncol, width),
                array(inner, cols, depth),
                array(tall, lots * size),
                array(lots, tall // 2, size),
                array(lots, nchip - 1, tall // (2 * nchip), size),
                array(lots, tall // (2 * nchip), size),
                array(lots, tall // (2 * nchip), size),
                pltpu.SemaphoreType.DMA((OUTER, 2, chunks)),
                pltpu.SemaphoreType.DMA((OUTER, chunks)),
                *pair(inner - 1, OUTER),
                *pair(chunks),
                *pair(chunks, nchip - 1),
                *pair(chunks, nchip - 1),
                *pair(chunks, nchip),
                *pair(chunks, OUTER - 1),
                *pair(chunks, nchip - 1),
                *pair(chunks, nchip),
                pltpu.SemaphoreType.DMA((OUTER + 1,)),
                *pair(inner),
                *pair(lots),
                *pair(lots, nchip - 1),
                *pair(lots),
            ],
            compiler_params=pltpu.CompilerParams(
                collective_id=0, has_side_effects=True, vmem_limit_bytes=VMEM
            ),
        )(matrix, basis)
        long = width // nrow
        part = lax.dynamic_slice(root, (0, lax.axis_index("row") * long), (width // ncol, long))
        return part.T, right

    return jax.shard_map(
        local,
        mesh=mesh,
        in_specs=(P("col", "row"), P(("row", "col"), None)),
        out_specs=(P("row", "col"), P("col", None)),
        check_vma=False,
    )
```

```python
import functools

import jax
import jax.numpy as jnp
from jax import lax
from jax.experimental import pallas as pl
from jax.experimental.pallas import tpu as pltpu
from jax.sharding import PartitionSpec as P

ITERS = 8
OUTER = 4
LANES = 128
VMEM = 62 * 1024 * 1024
MESH = pl.DeviceIdType.MESH


def split(x):
    hi = x.astype(jnp.bfloat16)
    lo = (x - hi.astype(jnp.float32)).astype(jnp.bfloat16)
    return hi, lo


def dot(a, b, dims=(((1,), (0,)), ((), ()))):
    return lax.dot_general(a, b, dimension_numbers=dims, preferred_element_type=jnp.float32)


def dot3(a, b, dims=(((1,), (0,)), ((), ()))):
    return dot(a[0], b[0], dims) + dot(a[0], b[1], dims) + dot(a[1], b[0], dims)


def kernel(
    nrow, ncol, size, taken, matrix, basis, root, right,
    slab, base, blocks, pieces, ahi, alo, total, halves, parts, plane, phi, plo, strip, strip_halves, strip_parts, shares, gram, work,
    given, lent, lent_halves, lent_parts, lent_sums, gifts,
    basis_send, basis_recv, piece_send, piece_recv, half_send, half_recv, part_send, part_recv,
    away_send, away_recv, mate_send, mate_recv, share_send, share_recv,
    gram_send, gram_recv, twin_send, twin_recv, load,
    given_send, given_recv, lent_half_send, lent_half_recv, lent_part_send, lent_part_recv, gift_send, gift_recv,
    strip_half_send, strip_half_recv, strip_part_send, strip_part_recv,
):
    inner = ncol // OUTER
    nchip = nrow // 2 * inner
    row, col = lax.axis_index("row"), lax.axis_index("col")
    out, inn = col // inner, lax.rem(col, inner)
    core = lax.rem(row, 2)
    chip = row // 2 * inner + inn
    me = core * nchip + chip
    cols, depth, width = matrix.shape[0], basis.shape[0], basis.shape[1]
    tall = plane.shape[0]
    high = tall // (2 * nchip)
    chunks = width // size
    thin = size // (2 * nchip)
    mate = {"row": row + 1 - 2 * core, "col": col}

    def chip_at(k):
        return lax.rem(chip + k, nchip)

    def from_chip(k):
        return lax.rem(chip + nchip - k, nchip)

    def chip_peer(k):
        other = chip_at(k)
        return {"row": other // inner * 2 + core, "col": out * inner + lax.rem(other, inner)}

    def line_peer(k):
        return {"row": row, "col": lax.rem(out + k, OUTER) * inner + inn}

    def remote(src, dst, send, recv, device):
        return pltpu.make_async_remote_copy(
            src_ref=src, dst_ref=dst, send_sem=send, recv_sem=recv, device_id=device, device_id_type=MESH
        )

    aside = out + 1 - 2 * lax.rem(out, 2)
    far = OUTER - 1 - out
    is_end = (out == 0) | (out == OUTER - 1)
    is_middle = (out > 0) & (out < OUTER - 1)
    aside_peer = {"row": row, "col": aside * inner + inn}

    def lanes(c):
        return pl.ds(c * size, size)

    def own_columns(at):
        return pl.ds(pl.multiple_of((at * inner + inn) * depth, depth), depth)

    loads = [pltpu.make_async_copy(basis, base, load.at[OUTER])]
    loads += [pltpu.make_async_copy(matrix.at[:, own_columns(at)], slab.at[at], load.at[at]) for at in range(OUTER)]
    for copy in loads:
        copy.start()
    barrier = pltpu.get_barrier_semaphore()
    greeted = [mate] + [chip_peer(k) for k in range(1, nchip)] + [line_peer(k) for k in range(1, OUTER)]
    for device in greeted:
        pl.semaphore_signal(barrier, inc=1, device_id=device, device_id_type=MESH)
    pl.semaphore_wait(barrier, len(greeted))

    def block_copy(source, step, c, own=False):
        here = blocks.at[source, :, lanes(c)]
        return remote(
            basis.at[:, lanes(c)] if own else here, here,
            basis_send.at[source, 0 if step > 0 else 1, c], basis_recv.at[source, c],
            {"row": row, "col": (out + step) * inner + inn},
        )

    def both_ways(step):
        return out < OUTER - 1 if step > 0 else out > 0

    def inside(source):
        return (source >= 0) & (source < OUTER)

    for step in (1, -1):
        @pl.when(both_ways(step))
        def _(step=step):
            for c in range(chunks):
                block_copy(out, step, c, True).start()

    def piece_copy(k, at):
        other = lax.rem(inn + k, inner)
        device = {"row": row, "col": out * inner + other}
        start = pl.multiple_of((at * inner + other) * depth, depth)
        return remote(
            matrix.at[:, pl.ds(start, depth)], pieces.at[k - 1, at],
            piece_send.at[k - 1, at], piece_recv.at[k - 1, at], device,
        )

    turn = [far, out, aside, OUTER - 1 - aside]
    for at in turn:
        for k in range(1, inner):
            piece_copy(k, at).start()

    def given_copy(k):
        start = pl.multiple_of((far * inner + inn) * depth, depth)
        return remote(
            pieces.at[k - 1, far] if k else matrix.at[:, pl.ds(start, depth)], given.at[k],
            given_send.at[k], given_recv.at[k], aside_peer,
        )

    if taken:
        @pl.when(is_end)
        def _():
            given_copy(0).start()

    def home(k):
        return pl.ds(pl.multiple_of(lax.rem(inn + inner - k, inner) * cols, cols), cols)

    def prepare(at, k):
        if k:
            piece_copy(k, at).wait_recv()
        ahi[at, home(k), :], alo[at, home(k), :] = split(pieces[k - 1, at] if k else slab[at])

    def add_block(at, block, where=slice(None), first=False):
        got = dot3((ahi[at], alo[at]), split(block[:, where]))
        total[:, where] = got if first else total[:, where] + got

    def pass_on(d, c):
        goes_on = d < OUTER - 2 or c not in taken
        for step in (1, -1):
            source = out - step * d

            @pl.when(inside(source))
            def _(source=source, step=step):
                block_copy(source, step, c).wait_recv()
                if goes_on:
                    @pl.when(both_ways(step))
                    def _():
                        block_copy(source, step, c).start()

    for copy in loads:
        copy.wait()
    for at in range(OUTER):
        prepare(at, 0)

    def add_turn(at, condition):
        def add():
            add_block(at, blocks.at[at])

        if condition is None:
            add()
        else:
            pl.when(condition)(add)

    for c in range(chunks):
        pass_on(1, c)
        if c == 0:
            for k in range(1, inner):
                prepare(far, k)
            if taken:
                @pl.when(is_end)
                def _():
                    for k in range(1, inner):
                        given_copy(k).start()
    for k in range(1, inner):
        prepare(out, k)
    add_block(out, base, first=True)
    add_turn(far, is_middle)
    for c in range(chunks):
        pass_on(2, c)
        if c == chunks // 2 - 1:
            for k in range(1, inner):
                prepare(aside, k)
            add_turn(aside, None)
    if chunks == 1:
        for k in range(1, inner):
            prepare(aside, k)
        add_turn(aside, None)
    for k in range(1, inner):
        prepare(OUTER - 1 - aside, k)
    if taken:
        @pl.when(is_middle)
        def _():
            for k in range(inner):
                given_copy(k).wait_recv()
                ahi[OUTER, home(k), :], alo[OUTER, home(k), :] = split(given[k])

    def lend(n):
        block = blocks[OUTER - 1 - aside, :, lanes(taken[n])]
        lent[:, lanes(n)] = dot3((ahi[OUTER], alo[OUTER]), split(block))

    def half(which):
        return pl.ds(pl.multiple_of(which * nchip * high, nchip * high), nchip * high)

    def part(which, at):
        return pl.ds(pl.multiple_of((which * nchip + at) * high, high), high)

    def half_copy(c):
        return remote(total.at[half(1 - core), lanes(c)], halves.at[c], half_send.at[c], half_recv.at[c], mate)

    def part_copy(c, k):
        return remote(
            total.at[part(core, chip_at(k)), lanes(c)], parts.at[c, k - 1],
            part_send.at[c, k - 1], part_recv.at[c, k - 1], chip_peer(k),
        )

    def lent_half_copy(n):
        return remote(
            lent.at[half(1 - core), lanes(n)], lent_halves.at[n], lent_half_send.at[n], lent_half_recv.at[n], mate
        )

    def lent_part_copy(n, k):
        return remote(
            lent.at[part(core, chip_at(k)), lanes(n)], lent_parts.at[n, k - 1],
            lent_part_send.at[n, k - 1], lent_part_recv.at[n, k - 1], chip_peer(k),
        )

    def gift_copy(n):
        return remote(lent_sums.at[n], gifts.at[n], gift_send.at[n], gift_recv.at[n], aside_peer)

    def lend_halves(n):
        lend(n)
        lent_half_copy(n).start()

    def lend_parts(n):
        lent_half_copy(n).wait_recv()
        lent[half(core), lanes(n)] = lent[half(core), lanes(n)] + lent_halves[n]
        for k in range(1, nchip):
            lent_part_copy(n, k).start()

    def give(n):
        mine = lent[part(core, chip), lanes(n)]
        for k in range(1, nchip):
            lent_part_copy(n, k).wait_recv()
            mine = mine + lent_parts[n, k - 1]
        lent_sums[n] = mine
        gift_copy(n).start()

    def gather(spot_of, send, recv, pair_send, pair_recv, wanted=None):
        def copy(which, at, c, send_sem, recv_sem, device):
            spot = spot_of(which, at, c)
            return remote(spot, spot, send_sem, recv_sem, device)

        def away(c, k, at):
            return copy(core, at, c, send.at[c, k - 1], recv.at[c, k - 1], chip_peer(k))

        def across(c, k, which):
            return copy(which, from_chip(k), c, pair_send.at[c, k], pair_recv.at[c, k], mate)

        def when(which, at, target):
            if wanted is None:
                return lambda act: act()
            return pl.when(wanted(which, at, lax.rem(target, inner)))

        def begin(c):
            for k in range(1, nchip):
                @when(core, chip, chip_at(k))
                def _(k=k):
                    away(c, k, chip).start()

            @when(core, chip, chip)
            def _():
                across(c, 0, core).start()

        def relay(c):
            for k in range(1, nchip):
                @when(core, from_chip(k), chip)
                def _(k=k):
                    away(c, k, from_chip(k)).wait_recv()
                    across(c, k, core).start()

        def end(c):
            for k in range(nchip):
                @when(1 - core, from_chip(k), chip)
                def _(k=k):
                    across(c, k, 1 - core).wait_recv()

        def finish(c):
            for k in range(1, nchip):
                @when(core, chip, chip_at(k))
                def _(k=k):
                    away(c, k, chip).wait_send()
            for k in range(nchip):
                @when(core, from_chip(k), chip)
                def _(k=k):
                    across(c, k, core).wait_send()

        return begin, relay, end, finish

    def columns_of(which, at, inner_at):
        return (which * nchip + at) * high // cols == inner_at

    def slim(which, at, c):
        return pl.ds(pl.multiple_of(c * size + (which * nchip + at) * thin, thin), thin)

    proj_begin, proj_relay, proj_end, proj_finish = gather(
        lambda which, at, c: plane.at[part(which, at), lanes(c)], away_send, away_recv, mate_send, mate_recv, columns_of
    )
    gram_begin, gram_relay, gram_end, gram_finish = gather(
        lambda which, at, c: gram.at[slim(which, at, c), pl.ds(0, (c + 1) * size)],
        gram_send, gram_recv, twin_send, twin_recv,
    )

    def share(c, slot):
        return shares.at[c, slot, :, pl.ds(0, (c + 1) * size)]

    def share_copy(c):
        return remote(share(c, 0), share(c, 1), share_send.at[c, 0], share_recv.at[c, 0], aside_peer)

    def pair_copy(c, n):
        plane_to = far if n == 0 else OUTER - 1 - aside
        device = {"row": row, "col": plane_to * inner + inn}
        return remote(share(c, 2), share(c, 3), share_send.at[c, 1 + n], share_recv.at[c, 1], device)

    def send_half(c):
        half_copy(c).start()

    def last_block(c):
        pass_on(OUTER - 1, c)
        add_block(far, blocks.at[far], lanes(c))
        send_half(c)

    def send_parts(c):
        half_copy(c).wait_recv()
        total[half(core), lanes(c)] = total[half(core), lanes(c)] + halves[c]
        for k in range(1, nchip):
            part_copy(c, k).start()

    def sum_parts(c, gift=None):
        mine = total[part(core, chip), lanes(c)]
        for k in range(1, nchip):
            part_copy(c, k).wait_recv()
            mine = mine + parts[c, k - 1]
        if gift is not None:
            gift_copy(gift).wait_recv()
            mine = mine + gifts[gift]
        plane[part(core, chip), lanes(c)] = mine
        local_gram(c, mine)

    def strip_half(which):
        return pl.ds(pl.multiple_of(which * nchip * thin, nchip * thin), nchip * thin)

    def strip_band(which, at):
        return pl.ds(pl.multiple_of((which * nchip + at) * thin, thin), thin)

    def strip_half_copy(c):
        wide = pl.ds(0, (c + 1) * size)
        return remote(
            strip.at[c, strip_half(1 - core), wide], strip_halves.at[c, :, wide],
            strip_half_send.at[c], strip_half_recv.at[c], mate,
        )

    def strip_part_copy(c, k):
        wide = pl.ds(0, (c + 1) * size)
        return remote(
            strip.at[c, strip_band(core, chip_at(k)), wide], strip_parts.at[c, k - 1, :, wide],
            strip_part_send.at[c, k - 1], strip_part_recv.at[c, k - 1], chip_peer(k),
        )

    def local_gram(c, mine):
        upto = (c + 1) * size
        some = split(mine)
        phi[:, lanes(c)], plo[:, lanes(c)] = some
        strip[c, :, 0:upto] = dot3(some, (phi[:, 0:upto], plo[:, 0:upto]), (((0,), (0,)), ((), ())))
        strip_half_copy(c).start()

    def send_strips(c):
        upto = (c + 1) * size
        strip_half_copy(c).wait_recv()
        strip[c, strip_half(core), 0:upto] = strip[c, strip_half(core), 0:upto] + strip_halves[c, :, 0:upto]
        for k in range(1, nchip):
            strip_part_copy(c, k).start()

    def send_gram(c):
        upto = (c + 1) * size
        mine = strip[c, strip_band(core, chip), 0:upto]
        for k in range(1, nchip):
            strip_part_copy(c, k).wait_recv()
            mine = mine + strip_parts[c, k - 1, :, 0:upto]
        shares[c, 0, :, 0:upto] = mine
        share_copy(c).start()

    def sum_pair(c):
        upto = (c + 1) * size
        share_copy(c).wait_recv()
        shares[c, 2, :, 0:upto] = shares[c, 0, :, 0:upto] + shares[c, 1, :, 0:upto]

    def send_pair(c):
        sum_pair(c)
        for n in range(2):
            pair_copy(c, n).start()

    def sum_gram(c):
        upto = (c + 1) * size
        pair_copy(c, 0).wait_recv()
        gram[slim(core, chip, c), 0:upto] = shares[c, 2, :, 0:upto] + shares[c, 3, :, 0:upto]
        gram_begin(c)

    squares = []

    def mirror(c):
        gram_end(c)
        square = gram[lanes(c), lanes(c)]
        square = 0.5 * (square + square.T)
        work[lanes(c), lanes(c)] = square
        squares.append(jnp.sum(square * square, keepdims=True))
        for b in range(c):
            block = gram[lanes(c), lanes(b)]
            work[lanes(c), lanes(b)] = block
            work[lanes(b), lanes(c)] = block.T
            squares.append(2.0 * jnp.sum(block * block, keepdims=True))

    def sum_with_gift(c):
        sum_parts(c, taken.index(c))

    last = OUTER - 1 - aside

    def add_last(where):
        add_block(last, blocks.at[last], where)

    if chunks == 4:
        end_order = [
            (add_last, slice(size, 3 * size)),
            (send_half, 1), (send_half, 2), (add_last, slice(0, size)), (add_last, slice(3 * size, width)),
            (send_parts, 1), (send_parts, 2), (last_block, 0), (send_parts, 0),
            (last_block, 3), (send_parts, 3), (sum_parts, 0), (sum_with_gift, 1), (send_strips, 0),
            (sum_with_gift, 2), (send_strips, 1), (sum_parts, 3), (send_strips, 2), (send_strips, 3),
        ]
        middle_order = [
            (add_last, slice(0, 2 * size)), (send_half, 0), (send_half, 1), (lend_halves, 0), (lend_halves, 1),
            (send_parts, 0), (add_last, slice(2 * size, width)), (send_half, 2), (send_half, 3), (lend_parts, 0),
            (lend_parts, 1), (send_parts, 1), (send_parts, 2), (send_parts, 3), (sum_parts, 0),
            (give, 0), (give, 1), (send_strips, 0), (sum_parts, 1), (sum_parts, 2), (send_strips, 1),
            (sum_parts, 3), (send_strips, 2), (send_strips, 3),
        ]
    else:
        lots = range(len(taken))
        each = range(chunks)
        end_order = [(add_last, slice(None))] + [(send_half if c in taken else last_block, c) for c in each]
        end_order += [(send_parts, c) for c in each]
        end_order += [(sum_with_gift if c in taken else sum_parts, c) for c in each]
        end_order += [(send_strips, c) for c in each]
        middle_order = [(add_last, slice(None))]
        middle_order += [(stage, n) for stage in (lend_halves, lend_parts, give) for n in lots]
        middle_order += [(stage, c) for stage in (send_half, send_parts, sum_parts, send_strips) for c in each]

    for role, order in ((is_end, end_order), (is_middle, middle_order)):
        order += [(proj_begin, c) for c in range(chunks)]
        for c in range(chunks + 1):
            if c < chunks:
                order.append((send_gram, c))
            if c and role is is_middle:
                order.append((send_pair, c - 1))
        for c in range(chunks):
            if role is is_end:
                order.append((sum_pair, c))
            order.append((sum_gram, c))

        @pl.when(role)
        def _(order=order):
            for stage, c in order:
                stage(c)

    for c in range(chunks + 1):
        if c < chunks:
            gram_relay(c)
        if c == chunks - 1:
            for past in range(chunks):
                proj_relay(past)
        if c:
            mirror(c - 1)

    scale = jnp.sqrt(sum(squares) + 1e-06)
    root_scale = jnp.sqrt(scale)
    per_scale = 1.0 / scale
    rows = root.shape[0]

    def halves_squared(x):
        cross = dot(x[0], x[1]).astype(jnp.bfloat16)
        return dot(x[0], x[0]) + (cross.astype(jnp.float32) + cross.T.astype(jnp.float32))

    for step in range(ITERS // 2):
        w = work[0:width, :]
        w_halves = split(w)
        e = halves_squared(w_halves)
        if step == 0:
            w = w * per_scale
            e = e * (per_scale * per_scale)
        e = e - 4.5 * w
        f = 0.0625 * halves_squared(split(e)) + (0.421875 * e - 0.5390625 * w)
        f_halves = split(f)
        if step == ITERS // 2 - 1:
            rest = work[width:, :]
            got = 2.25 * rest + dot3(split(rest), f_halves)
            right[...] = got[:cols, :] / root_scale
            root[...] = got[cols:, :] * root_scale
            break
        growth = split(halves_squared(f_halves) + 4.5 * f)
        if step == 0:
            for c in range(chunks):
                proj_end(c)
            work[width : width + cols, :] = plane[pl.ds(pl.multiple_of(inn * cols, cols), cols), :]
            work[width + cols :, :] = work[pl.ds(pl.multiple_of(col * rows, rows), rows), :] * per_scale
        rest = work[width:, :]
        work[width:, :] = 2.25 * rest + dot3(split(rest), f_halves)
        for start in range(0, width, LANES):
            band, after = slice(start, start + LANES), slice(start + LANES, width)
            product = dot3([half[band] for half in w_halves], [half[:, start:] for half in growth])
            if step == 0:
                product = product * per_scale
            square = product[:, :LANES]
            work[band, band] = 5.0625 * w[band, band] + 0.5 * (square + square.T)
            if start + LANES < width:
                work[band, after] = 5.0625 * w[band, after] + product[:, LANES:]
                work[after, band] = work[band, after].T

    for step in (1, -1):
        @pl.when(both_ways(step))
        def _(step=step):
            for c in range(chunks):
                block_copy(out, step, c, True).wait_send()
    for d in range(1, OUTER):
        for step in (1, -1):
            source = out - step * d

            @pl.when(inside(source) & both_ways(step))
            def _(source=source, step=step, d=d):
                for c in range(chunks):
                    if d < OUTER - 2 or c not in taken:
                        block_copy(source, step, c).wait_send()
    for at in turn:
        for k in range(1, inner):
            piece_copy(k, at).wait_send()
    if taken:
        @pl.when(is_end)
        def _():
            for k in range(inner):
                given_copy(k).wait_send()

        @pl.when(is_middle)
        def _():
            for n in range(len(taken)):
                lent_half_copy(n).wait_send()
                for k in range(1, nchip):
                    lent_part_copy(n, k).wait_send()
                gift_copy(n).wait_send()

    @pl.when(is_middle)
    def _():
        for c in range(chunks):
            for n in range(2):
                pair_copy(c, n).wait_send()

    for c in range(chunks):
        half_copy(c).wait_send()
        for k in range(1, nchip):
            part_copy(c, k).wait_send()
        share_copy(c).wait_send()
        strip_half_copy(c).wait_send()
        for k in range(1, nchip):
            strip_part_copy(c, k).wait_send()
        proj_finish(c)
        gram_finish(c)


def solution(mesh):
    nrow, ncol = mesh.shape["row"], mesh.shape["col"]
    inner = ncol // OUTER
    nchip = nrow // 2 * inner

    def local(matrix, basis):
        cols, (depth, width) = matrix.shape[0], basis.shape
        tall = inner * cols
        size = width if LANES % (16 * nchip) else LANES
        chunks = width // size
        taken = tuple(range(1, chunks - 1))
        lots = max(len(taken), 1)
        vmem = pl.BlockSpec(memory_space=pltpu.VMEM)

        def array(*shape, dtype=jnp.float32):
            return pltpu.VMEM(shape, dtype)

        def pair(*shape):
            return [pltpu.SemaphoreType.DMA(shape)] * 2

        root, right = pl.pallas_call(
            functools.partial(kernel, nrow, ncol, size, taken),
            out_shape=(
                array(width // ncol, width),
                array(cols, width),
            ),
            in_specs=[pl.BlockSpec(memory_space=pltpu.HBM)] * 2,
            out_specs=(vmem, vmem),
            scratch_shapes=[
                array(OUTER, cols, depth),
                array(depth, width),
                array(OUTER, depth, width),
                array(inner - 1, OUTER, cols, depth),
                array(OUTER + 1, tall, depth, dtype=jnp.bfloat16),
                array(OUTER + 1, tall, depth, dtype=jnp.bfloat16),
                array(tall, width),
                array(chunks, tall // 2, size),
                array(chunks, nchip - 1, tall // (2 * nchip), size),
                array(tall, width),
                array(tall // (2 * nchip), width, dtype=jnp.bfloat16),
                array(tall // (2 * nchip), width, dtype=jnp.bfloat16),
                array(chunks, size, width),
                array(chunks, size // 2, width),
                array(chunks, nchip - 1, size // (2 * nchip), width),
                array(chunks, OUTER, size // (2 * nchip), width),
                array(width, width),
                array(width + cols + width // ncol, width),
                array(inner, cols, depth),
                array(tall, lots * size),
                array(lots, tall // 2, size),
                array(lots, nchip - 1, tall // (2 * nchip), size),
                array(lots, tall // (2 * nchip), size),
                array(lots, tall // (2 * nchip), size),
                pltpu.SemaphoreType.DMA((OUTER, 2, chunks)),
                pltpu.SemaphoreType.DMA((OUTER, chunks)),
                *pair(inner - 1, OUTER),
                *pair(chunks),
                *pair(chunks, nchip - 1),
                *pair(chunks, nchip - 1),
                *pair(chunks, nchip),
                *pair(chunks, OUTER - 1),
                *pair(chunks, nchip - 1),
                *pair(chunks, nchip),
                pltpu.SemaphoreType.DMA((OUTER + 1,)),
                *pair(inner),
                *pair(lots),
                *pair(lots, nchip - 1),
                *pair(lots),
                *pair(chunks),
                *pair(chunks, nchip - 1),
            ],
            compiler_params=pltpu.CompilerParams(
                collective_id=0, has_side_effects=True, vmem_limit_bytes=VMEM
            ),
        )(matrix, basis)
        long = width // nrow
        part = lax.dynamic_slice(root, (0, lax.axis_index("row") * long), (width // ncol, long))
        return part.T, right

    return jax.shard_map(
        local,
        mesh=mesh,
        in_specs=(P("col", "row"), P(("row", "col"), None)),
        out_specs=(P("row", "col"), P("col", None)),
        check_vma=False,
    )
```

```python
import functools

import jax
import jax.numpy as jnp
from jax import lax
from jax.experimental import pallas as pl
from jax.experimental.pallas import tpu as pltpu
from jax.sharding import PartitionSpec as P

ITERS = 8
OUTER = 4
LANES = 128
VMEM = 62 * 1024 * 1024
MESH = pl.DeviceIdType.MESH


def split(x):
    hi = x.astype(jnp.bfloat16)
    lo = (x - hi.astype(jnp.float32)).astype(jnp.bfloat16)
    return hi, lo


def dot(a, b, dims=(((1,), (0,)), ((), ()))):
    return lax.dot_general(a, b, dimension_numbers=dims, preferred_element_type=jnp.float32)


def dot3(a, b, dims=(((1,), (0,)), ((), ()))):
    return dot(a[0], b[0], dims) + dot(a[0], b[1], dims) + dot(a[1], b[0], dims)


def kernel(
    nrow, ncol, size, taken, matrix, basis, root, right,
    slab, base, blocks, pieces, ahi, alo, total, halves, parts, plane, phi, plo, strip, strip_halves, strip_parts, shares, gram, work,
    given, lent, lent_halves, lent_parts, lent_sums, gifts,
    basis_send, basis_recv, piece_send, piece_recv, half_send, half_recv, part_send, part_recv,
    away_send, away_recv, mate_send, mate_recv, share_send, share_recv,
    gram_send, gram_recv, twin_send, twin_recv, load,
    given_send, given_recv, lent_half_send, lent_half_recv, lent_part_send, lent_part_recv, gift_send, gift_recv,
    strip_half_send, strip_half_recv, strip_part_send, strip_part_recv,
):
    inner = ncol // OUTER
    nchip = nrow // 2 * inner
    row, col = lax.axis_index("row"), lax.axis_index("col")
    out, inn = col // inner, lax.rem(col, inner)
    core = lax.rem(row, 2)
    chip = row // 2 * inner + inn
    me = core * nchip + chip
    cols, depth, width = matrix.shape[0], basis.shape[0], basis.shape[1]
    tall = plane.shape[0]
    high = tall // (2 * nchip)
    chunks = width // size
    thin = size // (2 * nchip)
    mate = {"row": row + 1 - 2 * core, "col": col}

    def chip_at(k):
        return lax.rem(chip + k, nchip)

    def from_chip(k):
        return lax.rem(chip + nchip - k, nchip)

    def chip_peer(k):
        other = chip_at(k)
        return {"row": other // inner * 2 + core, "col": out * inner + lax.rem(other, inner)}

    def line_peer(k):
        return {"row": row, "col": lax.rem(out + k, OUTER) * inner + inn}

    def remote(src, dst, send, recv, device):
        return pltpu.make_async_remote_copy(
            src_ref=src, dst_ref=dst, send_sem=send, recv_sem=recv, device_id=device, device_id_type=MESH
        )

    aside = out + 1 - 2 * lax.rem(out, 2)
    far = OUTER - 1 - out
    is_end = (out == 0) | (out == OUTER - 1)
    is_middle = (out > 0) & (out < OUTER - 1)
    aside_peer = {"row": row, "col": aside * inner + inn}

    def lanes(c):
        return pl.ds(c * size, size)

    def own_columns(at):
        return pl.ds(pl.multiple_of((at * inner + inn) * depth, depth), depth)

    loads = [pltpu.make_async_copy(basis, base, load.at[OUTER])]
    loads += [pltpu.make_async_copy(matrix.at[:, own_columns(at)], slab.at[at], load.at[at]) for at in range(OUTER)]
    for copy in loads:
        copy.start()
    barrier = pltpu.get_barrier_semaphore()
    greeted = [mate] + [chip_peer(k) for k in range(1, nchip)] + [line_peer(k) for k in range(1, OUTER)]
    for device in greeted:
        pl.semaphore_signal(barrier, inc=1, device_id=device, device_id_type=MESH)
    pl.semaphore_wait(barrier, len(greeted))

    def block_copy(source, step, c, own=False):
        here = blocks.at[source, :, lanes(c)]
        return remote(
            basis.at[:, lanes(c)] if own else here, here,
            basis_send.at[source, 0 if step > 0 else 1, c], basis_recv.at[source, c],
            {"row": row, "col": (out + step) * inner + inn},
        )

    def both_ways(step):
        return out < OUTER - 1 if step > 0 else out > 0

    def inside(source):
        return (source >= 0) & (source < OUTER)

    for step in (1, -1):
        @pl.when(both_ways(step))
        def _(step=step):
            for c in range(chunks):
                block_copy(out, step, c, True).start()

    def piece_copy(k, at):
        other = lax.rem(inn + k, inner)
        device = {"row": row, "col": out * inner + other}
        start = pl.multiple_of((at * inner + other) * depth, depth)
        return remote(
            matrix.at[:, pl.ds(start, depth)], pieces.at[k - 1, at],
            piece_send.at[k - 1, at], piece_recv.at[k - 1, at], device,
        )

    turn = [far, out, aside, OUTER - 1 - aside]
    for at in turn:
        for k in range(1, inner):
            piece_copy(k, at).start()

    def given_copy(k):
        start = pl.multiple_of((far * inner + inn) * depth, depth)
        return remote(
            pieces.at[k - 1, far] if k else matrix.at[:, pl.ds(start, depth)], given.at[k],
            given_send.at[k], given_recv.at[k], aside_peer,
        )

    if taken:
        @pl.when(is_end)
        def _():
            given_copy(0).start()

    def home(k):
        return pl.ds(pl.multiple_of(lax.rem(inn + inner - k, inner) * cols, cols), cols)

    def prepare(at, k):
        if k:
            piece_copy(k, at).wait_recv()
        ahi[at, home(k), :], alo[at, home(k), :] = split(pieces[k - 1, at] if k else slab[at])

    def add_block(at, block, where=slice(None), first=False):
        got = dot3((ahi[at], alo[at]), split(block[:, where]))
        total[:, where] = got if first else total[:, where] + got

    def pass_on(d, c):
        goes_on = d < OUTER - 2 or c not in taken
        for step in (1, -1):
            source = out - step * d

            @pl.when(inside(source))
            def _(source=source, step=step):
                block_copy(source, step, c).wait_recv()
                if goes_on:
                    @pl.when(both_ways(step))
                    def _():
                        block_copy(source, step, c).start()

    for copy in loads:
        copy.wait()
    for at in range(OUTER):
        prepare(at, 0)

    def add_turn(at, condition):
        def add():
            add_block(at, blocks.at[at])

        if condition is None:
            add()
        else:
            pl.when(condition)(add)

    for c in range(chunks):
        pass_on(1, c)
        if c == 0:
            for k in range(1, inner):
                prepare(far, k)
            if taken:
                @pl.when(is_end)
                def _():
                    for k in range(1, inner):
                        given_copy(k).start()
    for k in range(1, inner):
        prepare(out, k)
    add_block(out, base, first=True)
    add_turn(far, is_middle)
    for c in range(chunks):
        pass_on(2, c)
        if c == chunks // 2 - 1:
            for k in range(1, inner):
                prepare(aside, k)
            add_turn(aside, None)
    if chunks == 1:
        for k in range(1, inner):
            prepare(aside, k)
        add_turn(aside, None)
    for k in range(1, inner):
        prepare(OUTER - 1 - aside, k)
    if taken:
        @pl.when(is_middle)
        def _():
            for k in range(inner):
                given_copy(k).wait_recv()
                ahi[OUTER, home(k), :], alo[OUTER, home(k), :] = split(given[k])

    def lend(n):
        block = blocks[OUTER - 1 - aside, :, lanes(taken[n])]
        lent[:, lanes(n)] = dot3((ahi[OUTER], alo[OUTER]), split(block))

    def half(which):
        return pl.ds(pl.multiple_of(which * nchip * high, nchip * high), nchip * high)

    def part(which, at):
        return pl.ds(pl.multiple_of((which * nchip + at) * high, high), high)

    def half_copy(c):
        return remote(total.at[half(1 - core), lanes(c)], halves.at[c], half_send.at[c], half_recv.at[c], mate)

    def part_copy(c, k):
        return remote(
            total.at[part(core, chip_at(k)), lanes(c)], parts.at[c, k - 1],
            part_send.at[c, k - 1], part_recv.at[c, k - 1], chip_peer(k),
        )

    def lent_half_copy(n):
        return remote(
            lent.at[half(1 - core), lanes(n)], lent_halves.at[n], lent_half_send.at[n], lent_half_recv.at[n], mate
        )

    def lent_part_copy(n, k):
        return remote(
            lent.at[part(core, chip_at(k)), lanes(n)], lent_parts.at[n, k - 1],
            lent_part_send.at[n, k - 1], lent_part_recv.at[n, k - 1], chip_peer(k),
        )

    def gift_copy(n):
        return remote(lent_sums.at[n], gifts.at[n], gift_send.at[n], gift_recv.at[n], aside_peer)

    def lend_halves(n):
        lend(n)
        lent_half_copy(n).start()

    def lend_parts(n):
        lent_half_copy(n).wait_recv()
        lent[half(core), lanes(n)] = lent[half(core), lanes(n)] + lent_halves[n]
        for k in range(1, nchip):
            lent_part_copy(n, k).start()

    def give(n):
        mine = lent[part(core, chip), lanes(n)]
        for k in range(1, nchip):
            lent_part_copy(n, k).wait_recv()
            mine = mine + lent_parts[n, k - 1]
        lent_sums[n] = mine
        gift_copy(n).start()

    def gather(spot_of, send, recv, pair_send, pair_recv, wanted=None):
        def copy(which, at, c, send_sem, recv_sem, device):
            spot = spot_of(which, at, c)
            return remote(spot, spot, send_sem, recv_sem, device)

        def away(c, k, at):
            return copy(core, at, c, send.at[c, k - 1], recv.at[c, k - 1], chip_peer(k))

        def across(c, k, which):
            return copy(which, from_chip(k), c, pair_send.at[c, k], pair_recv.at[c, k], mate)

        def when(which, at, target):
            if wanted is None:
                return lambda act: act()
            return pl.when(wanted(which, at, lax.rem(target, inner)))

        def begin(c):
            for k in range(1, nchip):
                @when(core, chip, chip_at(k))
                def _(k=k):
                    away(c, k, chip).start()

            @when(core, chip, chip)
            def _():
                across(c, 0, core).start()

        def relay(c):
            for k in range(1, nchip):
                @when(core, from_chip(k), chip)
                def _(k=k):
                    away(c, k, from_chip(k)).wait_recv()
                    across(c, k, core).start()

        def end(c):
            for k in range(nchip):
                @when(1 - core, from_chip(k), chip)
                def _(k=k):
                    across(c, k, 1 - core).wait_recv()

        def finish(c):
            for k in range(1, nchip):
                @when(core, chip, chip_at(k))
                def _(k=k):
                    away(c, k, chip).wait_send()
            for k in range(nchip):
                @when(core, from_chip(k), chip)
                def _(k=k):
                    across(c, k, core).wait_send()

        return begin, relay, end, finish

    def columns_of(which, at, inner_at):
        return (which * nchip + at) * high // cols == inner_at

    def slim(which, at, c):
        return pl.ds(pl.multiple_of(c * size + (which * nchip + at) * thin, thin), thin)

    proj_begin, proj_relay, proj_end, proj_finish = gather(
        lambda which, at, c: plane.at[part(which, at), lanes(c)], away_send, away_recv, mate_send, mate_recv, columns_of
    )
    gram_begin, gram_relay, gram_end, gram_finish = gather(
        lambda which, at, c: gram.at[slim(which, at, c), pl.ds(0, (c + 1) * size)],
        gram_send, gram_recv, twin_send, twin_recv,
    )

    def share(c, slot):
        return shares.at[c, slot, :, pl.ds(0, (c + 1) * size)]

    def share_copy(c):
        return remote(share(c, 0), share(c, 1), share_send.at[c, 0], share_recv.at[c, 0], aside_peer)

    def pair_copy(c, n):
        plane_to = far if n == 0 else OUTER - 1 - aside
        device = {"row": row, "col": plane_to * inner + inn}
        return remote(share(c, 2), share(c, 3), share_send.at[c, 1 + n], share_recv.at[c, 1], device)

    def send_half(c):
        half_copy(c).start()

    def last_block(c):
        pass_on(OUTER - 1, c)
        add_block(far, blocks.at[far], lanes(c))
        send_half(c)

    def send_parts(c):
        half_copy(c).wait_recv()
        total[half(core), lanes(c)] = total[half(core), lanes(c)] + halves[c]
        for k in range(1, nchip):
            part_copy(c, k).start()

    def sum_parts(c, gift=None):
        mine = total[part(core, chip), lanes(c)]
        for k in range(1, nchip):
            part_copy(c, k).wait_recv()
            mine = mine + parts[c, k - 1]
        if gift is not None:
            gift_copy(gift).wait_recv()
            mine = mine + gifts[gift]
        plane[part(core, chip), lanes(c)] = mine
        local_gram(c, mine)

    def strip_half(which):
        return pl.ds(pl.multiple_of(which * nchip * thin, nchip * thin), nchip * thin)

    def strip_band(which, at):
        return pl.ds(pl.multiple_of((which * nchip + at) * thin, thin), thin)

    def strip_half_copy(c):
        wide = pl.ds(0, (c + 1) * size)
        return remote(
            strip.at[c, strip_half(1 - core), wide], strip_halves.at[c, :, wide],
            strip_half_send.at[c], strip_half_recv.at[c], mate,
        )

    def strip_part_copy(c, k):
        wide = pl.ds(0, (c + 1) * size)
        return remote(
            strip.at[c, strip_band(core, chip_at(k)), wide], strip_parts.at[c, k - 1, :, wide],
            strip_part_send.at[c, k - 1], strip_part_recv.at[c, k - 1], chip_peer(k),
        )

    def local_gram(c, mine):
        upto = (c + 1) * size
        some = split(mine)
        phi[:, lanes(c)], plo[:, lanes(c)] = some
        strip[c, :, 0:upto] = dot3(some, (phi[:, 0:upto], plo[:, 0:upto]), (((0,), (0,)), ((), ())))
        strip_half_copy(c).start()

    def send_strips(c):
        upto = (c + 1) * size
        strip_half_copy(c).wait_recv()
        strip[c, strip_half(core), 0:upto] = strip[c, strip_half(core), 0:upto] + strip_halves[c, :, 0:upto]
        for k in range(1, nchip):
            strip_part_copy(c, k).start()

    def send_gram(c):
        upto = (c + 1) * size
        mine = strip[c, strip_band(core, chip), 0:upto]
        for k in range(1, nchip):
            strip_part_copy(c, k).wait_recv()
            mine = mine + strip_parts[c, k - 1, :, 0:upto]
        shares[c, 0, :, 0:upto] = mine
        share_copy(c).start()

    def sum_pair(c):
        upto = (c + 1) * size
        share_copy(c).wait_recv()
        shares[c, 2, :, 0:upto] = shares[c, 0, :, 0:upto] + shares[c, 1, :, 0:upto]

    def send_pair(c):
        sum_pair(c)
        for n in range(2):
            pair_copy(c, n).start()

    def sum_gram(c):
        upto = (c + 1) * size
        pair_copy(c, 0).wait_recv()
        gram[slim(core, chip, c), 0:upto] = shares[c, 2, :, 0:upto] + shares[c, 3, :, 0:upto]
        gram_begin(c)

    squares = []

    def mirror(c):
        gram_end(c)
        square = gram[lanes(c), lanes(c)]
        square = 0.5 * (square + square.T)
        work[lanes(c), lanes(c)] = square
        squares.append(jnp.sum(square * square, keepdims=True))
        for b in range(c):
            block = gram[lanes(c), lanes(b)]
            work[lanes(c), lanes(b)] = block
            work[lanes(b), lanes(c)] = block.T
            squares.append(2.0 * jnp.sum(block * block, keepdims=True))

    def sum_with_gift(c):
        sum_parts(c, taken.index(c))

    last = OUTER - 1 - aside

    def add_last(where):
        add_block(last, blocks.at[last], where)

    if chunks == 4:
        end_order = [
            (add_last, slice(size, 3 * size)),
            (send_half, 1), (send_half, 2), (add_last, slice(0, size)), (add_last, slice(3 * size, width)),
            (send_parts, 1), (send_parts, 2), (last_block, 0), (send_parts, 0),
            (last_block, 3), (send_parts, 3), (sum_parts, 0), (sum_with_gift, 1), (send_strips, 0),
            (sum_with_gift, 2), (send_strips, 1), (sum_parts, 3), (send_strips, 2), (send_strips, 3),
        ]
        middle_order = [
            (add_last, slice(0, size)), (send_half, 0), (lend_halves, 0), (lend_halves, 1), (send_parts, 0),
            (add_last, slice(size, width)), (send_half, 1), (send_half, 2), (send_half, 3), (lend_parts, 0),
            (lend_parts, 1), (send_parts, 1), (send_parts, 2), (send_parts, 3), (sum_parts, 0),
            (give, 0), (give, 1), (send_strips, 0), (sum_parts, 1), (sum_parts, 2), (send_strips, 1),
            (sum_parts, 3), (send_strips, 2), (send_strips, 3),
        ]
    else:
        lots = range(len(taken))
        each = range(chunks)
        end_order = [(add_last, slice(None))] + [(send_half if c in taken else last_block, c) for c in each]
        end_order += [(send_parts, c) for c in each]
        end_order += [(sum_with_gift if c in taken else sum_parts, c) for c in each]
        end_order += [(send_strips, c) for c in each]
        middle_order = [(add_last, slice(None))]
        middle_order += [(stage, n) for stage in (lend_halves, lend_parts, give) for n in lots]
        middle_order += [(stage, c) for stage in (send_half, send_parts, sum_parts, send_strips) for c in each]

    for role, order in ((is_end, end_order), (is_middle, middle_order)):
        order += [(proj_begin, c) for c in range(chunks)]
        for c in range(chunks + 1):
            if c < chunks:
                order.append((send_gram, c))
            if c and role is is_middle:
                order.append((send_pair, c - 1))
        for c in range(chunks):
            if role is is_end:
                order.append((sum_pair, c))
            order.append((sum_gram, c))

        @pl.when(role)
        def _(order=order):
            for stage, c in order:
                stage(c)

    for step in (1, -1):
        @pl.when(both_ways(step))
        def _(step=step):
            for c in range(chunks):
                block_copy(out, step, c, True).wait_send()
    for d in range(1, OUTER):
        for step in (1, -1):
            source = out - step * d

            @pl.when(inside(source) & both_ways(step))
            def _(source=source, step=step, d=d):
                for c in range(chunks):
                    if d < OUTER - 2 or c not in taken:
                        block_copy(source, step, c).wait_send()
    for at in turn:
        for k in range(1, inner):
            piece_copy(k, at).wait_send()
    if taken:
        @pl.when(is_end)
        def _():
            for k in range(inner):
                given_copy(k).wait_send()

        @pl.when(is_middle)
        def _():
            for n in range(len(taken)):
                lent_half_copy(n).wait_send()
                for k in range(1, nchip):
                    lent_part_copy(n, k).wait_send()
                gift_copy(n).wait_send()

    @pl.when(is_middle)
    def _():
        for c in range(chunks):
            for n in range(2):
                pair_copy(c, n).wait_send()

    for c in range(chunks):
        half_copy(c).wait_send()
        for k in range(1, nchip):
            part_copy(c, k).wait_send()
        share_copy(c).wait_send()
        strip_half_copy(c).wait_send()
        for k in range(1, nchip):
            strip_part_copy(c, k).wait_send()

    for c in range(chunks + 1):
        if c < chunks:
            gram_relay(c)
        if c == chunks - 1:
            for past in range(chunks):
                proj_relay(past)
        if c:
            mirror(c - 1)

    scale = jnp.sqrt(sum(squares) + 1e-06)
    root_scale = jnp.sqrt(scale)
    per_scale = 1.0 / scale
    rows = root.shape[0]

    def halves_squared(x):
        cross = dot(x[0], x[1]).astype(jnp.bfloat16)
        return dot(x[0], x[0]) + (cross.astype(jnp.float32) + cross.T.astype(jnp.float32))

    for step in range(ITERS // 2):
        w = work[0:width, :]
        w_halves = split(w)
        e = halves_squared(w_halves)
        if step == 0:
            w = w * per_scale
            e = e * (per_scale * per_scale)
        e = e - 4.5 * w
        f = 0.0625 * halves_squared(split(e)) + (0.421875 * e - 0.5390625 * w)
        f_halves = split(f)
        if step == ITERS // 2 - 1:
            rest = work[width:, :]
            got = 2.25 * rest + dot3(split(rest), f_halves)
            right[...] = got[:cols, :] * (1.0 / root_scale)
            if root.shape[1] == width:
                root[...] = got[cols:, :] * root_scale
            else:
                work[width + cols :, :] = got[cols:, :]
                long = root.shape[1]
                root[...] = work[width + cols :, pl.ds(pl.multiple_of(row * long, long), long)] * root_scale
            break
        growth = split(halves_squared(f_halves) + 4.5 * f)
        if step == 0:
            for c in range(chunks):
                proj_end(c)
            work[width : width + cols, :] = plane[pl.ds(pl.multiple_of(inn * cols, cols), cols), :]
            work[width + cols :, :] = work[pl.ds(pl.multiple_of(col * rows, rows), rows), :] * per_scale
        rest = work[width:, :]
        work[width:, :] = 2.25 * rest + dot3(split(rest), f_halves)
        for start in range(0, width, LANES):
            band, after = slice(start, start + LANES), slice(start + LANES, width)
            product = dot3([half[band] for half in w_halves], [half[:, start:] for half in growth])
            if step == 0:
                product = product * per_scale
            square = product[:, :LANES]
            work[band, band] = 5.0625 * w[band, band] + 0.5 * (square + square.T)
            if start + LANES < width:
                work[band, after] = 5.0625 * w[band, after] + product[:, LANES:]
                work[after, band] = work[band, after].T

    for c in range(chunks):
        proj_finish(c)
        gram_finish(c)


def solution(mesh):
    nrow, ncol = mesh.shape["row"], mesh.shape["col"]
    inner = ncol // OUTER
    nchip = nrow // 2 * inner

    def local(matrix, basis):
        cols, (depth, width) = matrix.shape[0], basis.shape
        tall = inner * cols
        size = width if LANES % (16 * nchip) else LANES
        chunks = width // size
        taken = tuple(range(1, chunks - 1))
        lots = max(len(taken), 1)
        vmem = pl.BlockSpec(memory_space=pltpu.VMEM)

        def array(*shape, dtype=jnp.float32):
            return pltpu.VMEM(shape, dtype)

        def pair(*shape):
            return [pltpu.SemaphoreType.DMA(shape)] * 2

        long = width // nrow
        root, right = pl.pallas_call(
            functools.partial(kernel, nrow, ncol, size, taken),
            out_shape=(
                array(width // ncol, width if long % LANES else long),
                array(cols, width),
            ),
            in_specs=[pl.BlockSpec(memory_space=pltpu.HBM)] * 2,
            out_specs=(vmem, vmem),
            scratch_shapes=[
                array(OUTER, cols, depth),
                array(depth, width),
                array(OUTER, depth, width),
                array(inner - 1, OUTER, cols, depth),
                array(OUTER + 1, tall, depth, dtype=jnp.bfloat16),
                array(OUTER + 1, tall, depth, dtype=jnp.bfloat16),
                array(tall, width),
                array(chunks, tall // 2, size),
                array(chunks, nchip - 1, tall // (2 * nchip), size),
                array(tall, width),
                array(tall // (2 * nchip), width, dtype=jnp.bfloat16),
                array(tall // (2 * nchip), width, dtype=jnp.bfloat16),
                array(chunks, size, width),
                array(chunks, size // 2, width),
                array(chunks, nchip - 1, size // (2 * nchip), width),
                array(chunks, OUTER, size // (2 * nchip), width),
                array(width, width),
                array(width + cols + width // ncol, width),
                array(inner, cols, depth),
                array(tall, lots * size),
                array(lots, tall // 2, size),
                array(lots, nchip - 1, tall // (2 * nchip), size),
                array(lots, tall // (2 * nchip), size),
                array(lots, tall // (2 * nchip), size),
                pltpu.SemaphoreType.DMA((OUTER, 2, chunks)),
                pltpu.SemaphoreType.DMA((OUTER, chunks)),
                *pair(inner - 1, OUTER),
                *pair(chunks),
                *pair(chunks, nchip - 1),
                *pair(chunks, nchip - 1),
                *pair(chunks, nchip),
                *pair(chunks, OUTER - 1),
                *pair(chunks, nchip - 1),
                *pair(chunks, nchip),
                pltpu.SemaphoreType.DMA((OUTER + 1,)),
                *pair(inner),
                *pair(lots),
                *pair(lots, nchip - 1),
                *pair(lots),
                *pair(chunks),
                *pair(chunks, nchip - 1),
            ],
            compiler_params=pltpu.CompilerParams(
                collective_id=0, has_side_effects=True, vmem_limit_bytes=VMEM
            ),
        )(matrix, basis)
        if long % LANES == 0:
            return root.T, right
        part = lax.dynamic_slice(root, (0, lax.axis_index("row") * long), (width // ncol, long))
        return part.T, right

    return jax.shard_map(
        local,
        mesh=mesh,
        in_specs=(P("col", "row"), P(("row", "col"), None)),
        out_specs=(P("row", "col"), P("col", None)),
        check_vma=False,
    )
```

```python
import functools

import jax
import jax.numpy as jnp
from jax import lax
from jax.experimental import pallas as pl
from jax.experimental.pallas import tpu as pltpu
from jax.sharding import PartitionSpec as P

ITERS = 8
OUTER = 4
LANES = 128
VMEM = 62 * 1024 * 1024
MESH = pl.DeviceIdType.MESH


def split(x):
    hi = x.astype(jnp.bfloat16)
    lo = (x - hi.astype(jnp.float32)).astype(jnp.bfloat16)
    return hi, lo


def dot(a, b, dims=(((1,), (0,)), ((), ()))):
    return lax.dot_general(a, b, dimension_numbers=dims, preferred_element_type=jnp.float32)


def dot3(a, b, dims=(((1,), (0,)), ((), ()))):
    return dot(a[0], b[0], dims) + dot(a[0], b[1], dims) + dot(a[1], b[0], dims)


def kernel(
    nrow, ncol, size, taken, matrix, basis, root, right,
    slab, base, blocks, pieces, ahi, alo, total, halves, parts, plane, phi, plo, strip, strip_halves, strip_parts, shares, gram, work,
    given, lent, lent_halves, lent_parts, lent_sums, gifts,
    basis_send, basis_recv, piece_send, piece_recv, half_send, half_recv, part_send, part_recv,
    away_send, away_recv, mate_send, mate_recv, share_send, share_recv,
    gram_send, gram_recv, twin_send, twin_recv, load,
    given_send, given_recv, lent_half_send, lent_half_recv, lent_part_send, lent_part_recv, gift_send, gift_recv,
    strip_half_send, strip_half_recv, strip_part_send, strip_part_recv,
):
    inner = ncol // OUTER
    nchip = nrow // 2 * inner
    row, col = lax.axis_index("row"), lax.axis_index("col")
    out, inn = col // inner, lax.rem(col, inner)
    core = lax.rem(row, 2)
    chip = row // 2 * inner + inn
    me = core * nchip + chip
    cols, depth, width = matrix.shape[0], basis.shape[0], basis.shape[1]
    tall = plane.shape[0]
    high = tall // (2 * nchip)
    chunks = width // size
    thin = size // (2 * nchip)
    mate = {"row": row + 1 - 2 * core, "col": col}

    def chip_at(k):
        return lax.rem(chip + k, nchip)

    def from_chip(k):
        return lax.rem(chip + nchip - k, nchip)

    def chip_peer(k):
        other = chip_at(k)
        return {"row": other // inner * 2 + core, "col": out * inner + lax.rem(other, inner)}

    def line_peer(k):
        return {"row": row, "col": lax.rem(out + k, OUTER) * inner + inn}

    def remote(src, dst, send, recv, device):
        return pltpu.make_async_remote_copy(
            src_ref=src, dst_ref=dst, send_sem=send, recv_sem=recv, device_id=device, device_id_type=MESH
        )

    aside = out + 1 - 2 * lax.rem(out, 2)
    far = OUTER - 1 - out
    is_end = (out == 0) | (out == OUTER - 1)
    is_middle = (out > 0) & (out < OUTER - 1)
    aside_peer = {"row": row, "col": aside * inner + inn}

    def lanes(c):
        return pl.ds(c * size, size)

    def own_columns(at):
        return pl.ds(pl.multiple_of((at * inner + inn) * depth, depth), depth)

    loads = [pltpu.make_async_copy(basis, base, load.at[OUTER])]
    loads += [pltpu.make_async_copy(matrix.at[:, own_columns(at)], slab.at[at], load.at[at]) for at in range(OUTER)]
    for copy in loads:
        copy.start()
    barrier = pltpu.get_barrier_semaphore()
    greeted = [mate] + [chip_peer(k) for k in range(1, nchip)] + [line_peer(k) for k in range(1, OUTER)]
    for device in greeted:
        pl.semaphore_signal(barrier, inc=1, device_id=device, device_id_type=MESH)
    pl.semaphore_wait(barrier, len(greeted))

    def block_copy(source, step, c, own=False):
        here = blocks.at[source, :, lanes(c)]
        return remote(
            basis.at[:, lanes(c)] if own else here, here,
            basis_send.at[source, 0 if step > 0 else 1, c], basis_recv.at[source, c],
            {"row": row, "col": (out + step) * inner + inn},
        )

    def both_ways(step):
        return out < OUTER - 1 if step > 0 else out > 0

    def inside(source):
        return (source >= 0) & (source < OUTER)

    for step in (1, -1):
        @pl.when(both_ways(step))
        def _(step=step):
            for c in range(chunks):
                block_copy(out, step, c, True).start()

    def piece_copy(k, at):
        other = lax.rem(inn + k, inner)
        device = {"row": row, "col": out * inner + other}
        start = pl.multiple_of((at * inner + other) * depth, depth)
        return remote(
            matrix.at[:, pl.ds(start, depth)], pieces.at[k - 1, at],
            piece_send.at[k - 1, at], piece_recv.at[k - 1, at], device,
        )

    turn = [far, out, aside, OUTER - 1 - aside]
    for at in turn:
        for k in range(1, inner):
            piece_copy(k, at).start()

    def given_copy(k):
        start = pl.multiple_of((far * inner + inn) * depth, depth)
        return remote(
            pieces.at[k - 1, far] if k else matrix.at[:, pl.ds(start, depth)], given.at[k],
            given_send.at[k], given_recv.at[k], aside_peer,
        )

    if taken:
        @pl.when(is_end)
        def _():
            given_copy(0).start()

    def home(k):
        return pl.ds(pl.multiple_of(lax.rem(inn + inner - k, inner) * cols, cols), cols)

    def prepare(at, k):
        if k:
            piece_copy(k, at).wait_recv()
        ahi[at, home(k), :], alo[at, home(k), :] = split(pieces[k - 1, at] if k else slab[at])

    def add_block(at, block, where=slice(None), first=False):
        got = dot3((ahi[at], alo[at]), split(block[:, where]))
        total[:, where] = got if first else total[:, where] + got

    def pass_on(d, c):
        goes_on = d < OUTER - 2 or c not in taken
        for step in (1, -1):
            source = out - step * d

            @pl.when(inside(source))
            def _(source=source, step=step):
                block_copy(source, step, c).wait_recv()
                if goes_on:
                    @pl.when(both_ways(step))
                    def _():
                        block_copy(source, step, c).start()

    for copy in loads:
        copy.wait()
    for at in range(OUTER):
        prepare(at, 0)

    def add_turn(at, condition):
        def add():
            add_block(at, blocks.at[at])

        if condition is None:
            add()
        else:
            pl.when(condition)(add)

    for c in range(chunks):
        pass_on(1, c)
        if c == 0:
            for k in range(1, inner):
                prepare(far, k)
            if taken:
                @pl.when(is_end)
                def _():
                    for k in range(1, inner):
                        given_copy(k).start()
    for k in range(1, inner):
        prepare(out, k)
    add_block(out, base, first=True)
    add_turn(far, is_middle)
    for c in range(chunks):
        pass_on(2, c)
        if c == chunks // 2 - 1:
            for k in range(1, inner):
                prepare(aside, k)
            add_turn(aside, None)
    if chunks == 1:
        for k in range(1, inner):
            prepare(aside, k)
        add_turn(aside, None)
    for k in range(1, inner):
        prepare(OUTER - 1 - aside, k)
    if taken:
        @pl.when(is_middle)
        def _():
            for k in range(inner):
                given_copy(k).wait_recv()
                ahi[OUTER, home(k), :], alo[OUTER, home(k), :] = split(given[k])

    def lend(n):
        block = blocks[OUTER - 1 - aside, :, lanes(taken[n])]
        lent[:, lanes(n)] = dot3((ahi[OUTER], alo[OUTER]), split(block))

    def half(which):
        return pl.ds(pl.multiple_of(which * nchip * high, nchip * high), nchip * high)

    def part(which, at):
        return pl.ds(pl.multiple_of((which * nchip + at) * high, high), high)

    def half_copy(c):
        return remote(total.at[half(1 - core), lanes(c)], halves.at[c], half_send.at[c], half_recv.at[c], mate)

    def part_copy(c, k):
        return remote(
            total.at[part(core, chip_at(k)), lanes(c)], parts.at[c, k - 1],
            part_send.at[c, k - 1], part_recv.at[c, k - 1], chip_peer(k),
        )

    def lent_half_copy(n):
        return remote(
            lent.at[half(1 - core), lanes(n)], lent_halves.at[n], lent_half_send.at[n], lent_half_recv.at[n], mate
        )

    def lent_part_copy(n, k):
        return remote(
            lent.at[part(core, chip_at(k)), lanes(n)], lent_parts.at[n, k - 1],
            lent_part_send.at[n, k - 1], lent_part_recv.at[n, k - 1], chip_peer(k),
        )

    def gift_copy(n):
        return remote(lent_sums.at[n], gifts.at[n], gift_send.at[n], gift_recv.at[n], aside_peer)

    def lend_halves(n):
        lend(n)
        lent_half_copy(n).start()

    def lend_parts(n):
        lent_half_copy(n).wait_recv()
        lent[half(core), lanes(n)] = lent[half(core), lanes(n)] + lent_halves[n]
        for k in range(1, nchip):
            lent_part_copy(n, k).start()

    def give(n):
        mine = lent[part(core, chip), lanes(n)]
        for k in range(1, nchip):
            lent_part_copy(n, k).wait_recv()
            mine = mine + lent_parts[n, k - 1]
        lent_sums[n] = mine
        gift_copy(n).start()

    def gather(spot_of, send, recv, pair_send, pair_recv, wanted=None):
        def copy(which, at, c, send_sem, recv_sem, device):
            spot = spot_of(which, at, c)
            return remote(spot, spot, send_sem, recv_sem, device)

        def away(c, k, at):
            return copy(core, at, c, send.at[c, k - 1], recv.at[c, k - 1], chip_peer(k))

        def across(c, k, which):
            return copy(which, from_chip(k), c, pair_send.at[c, k], pair_recv.at[c, k], mate)

        def when(which, at, target):
            if wanted is None:
                return lambda act: act()
            return pl.when(wanted(which, at, lax.rem(target, inner)))

        def begin(c):
            for k in range(1, nchip):
                @when(core, chip, chip_at(k))
                def _(k=k):
                    away(c, k, chip).start()

            @when(core, chip, chip)
            def _():
                across(c, 0, core).start()

        def relay(c):
            for k in range(1, nchip):
                @when(core, from_chip(k), chip)
                def _(k=k):
                    away(c, k, from_chip(k)).wait_recv()
                    across(c, k, core).start()

        def end(c):
            for k in range(nchip):
                @when(1 - core, from_chip(k), chip)
                def _(k=k):
                    across(c, k, 1 - core).wait_recv()

        def finish(c):
            for k in range(1, nchip):
                @when(core, chip, chip_at(k))
                def _(k=k):
                    away(c, k, chip).wait_send()
            for k in range(nchip):
                @when(core, from_chip(k), chip)
                def _(k=k):
                    across(c, k, core).wait_send()

        return begin, relay, end, finish

    def columns_of(which, at, inner_at):
        return (which * nchip + at) * high // cols == inner_at

    def slim(which, at, c):
        return pl.ds(pl.multiple_of(c * size + (which * nchip + at) * thin, thin), thin)

    proj_begin, proj_relay, proj_end, proj_finish = gather(
        lambda which, at, c: plane.at[part(which, at), lanes(c)], away_send, away_recv, mate_send, mate_recv, columns_of
    )
    gram_begin, gram_relay, gram_end, gram_finish = gather(
        lambda which, at, c: gram.at[slim(which, at, c), pl.ds(0, (c + 1) * size)],
        gram_send, gram_recv, twin_send, twin_recv,
    )

    def share(c, slot):
        return shares.at[c, slot, :, pl.ds(0, (c + 1) * size)]

    def share_copy(c):
        return remote(share(c, 0), share(c, 1), share_send.at[c, 0], share_recv.at[c, 0], aside_peer)

    def pair_copy(c, n):
        plane_to = far if n == 0 else OUTER - 1 - aside
        device = {"row": row, "col": plane_to * inner + inn}
        return remote(share(c, 2), share(c, 3), share_send.at[c, 1 + n], share_recv.at[c, 1], device)

    def send_half(c):
        half_copy(c).start()

    def last_block(c):
        pass_on(OUTER - 1, c)
        add_block(far, blocks.at[far], lanes(c))
        send_half(c)

    def send_parts(c):
        half_copy(c).wait_recv()
        total[half(core), lanes(c)] = total[half(core), lanes(c)] + halves[c]
        for k in range(1, nchip):
            part_copy(c, k).start()

    def sum_parts(c, gift=None):
        mine = total[part(core, chip), lanes(c)]
        for k in range(1, nchip):
            part_copy(c, k).wait_recv()
            mine = mine + parts[c, k - 1]
        if gift is not None:
            gift_copy(gift).wait_recv()
            mine = mine + gifts[gift]
        plane[part(core, chip), lanes(c)] = mine
        local_gram(c, mine)

    def strip_half(which):
        return pl.ds(pl.multiple_of(which * nchip * thin, nchip * thin), nchip * thin)

    def strip_band(which, at):
        return pl.ds(pl.multiple_of((which * nchip + at) * thin, thin), thin)

    def strip_half_copy(c):
        wide = pl.ds(0, (c + 1) * size)
        return remote(
            strip.at[c, strip_half(1 - core), wide], strip_halves.at[c, :, wide],
            strip_half_send.at[c], strip_half_recv.at[c], mate,
        )

    def strip_part_copy(c, k):
        wide = pl.ds(0, (c + 1) * size)
        return remote(
            strip.at[c, strip_band(core, chip_at(k)), wide], strip_parts.at[c, k - 1, :, wide],
            strip_part_send.at[c, k - 1], strip_part_recv.at[c, k - 1], chip_peer(k),
        )

    def local_gram(c, mine):
        upto = (c + 1) * size
        some = split(mine)
        phi[:, lanes(c)], plo[:, lanes(c)] = some
        strip[c, :, 0:upto] = dot3(some, (phi[:, 0:upto], plo[:, 0:upto]), (((0,), (0,)), ((), ())))
        strip_half_copy(c).start()

    def send_strips(c):
        upto = (c + 1) * size
        strip_half_copy(c).wait_recv()
        strip[c, strip_half(core), 0:upto] = strip[c, strip_half(core), 0:upto] + strip_halves[c, :, 0:upto]
        for k in range(1, nchip):
            strip_part_copy(c, k).start()

    def send_gram(c):
        upto = (c + 1) * size
        mine = strip[c, strip_band(core, chip), 0:upto]
        for k in range(1, nchip):
            strip_part_copy(c, k).wait_recv()
            mine = mine + strip_parts[c, k - 1, :, 0:upto]
        shares[c, 0, :, 0:upto] = mine
        share_copy(c).start()

    def sum_pair(c):
        upto = (c + 1) * size
        share_copy(c).wait_recv()
        shares[c, 2, :, 0:upto] = shares[c, 0, :, 0:upto] + shares[c, 1, :, 0:upto]

    def send_pair(c):
        sum_pair(c)
        for n in range(2):
            pair_copy(c, n).start()

    def sum_gram(c):
        upto = (c + 1) * size
        pair_copy(c, 0).wait_recv()
        gram[slim(core, chip, c), 0:upto] = shares[c, 2, :, 0:upto] + shares[c, 3, :, 0:upto]
        gram_begin(c)

    squares = []

    def mirror(c):
        gram_end(c)
        square = gram[lanes(c), lanes(c)]
        square = 0.5 * (square + square.T)
        work[lanes(c), lanes(c)] = square
        squares.append(square * square)
        for b in range(c):
            block = gram[lanes(c), lanes(b)]
            work[lanes(c), lanes(b)] = block
            work[lanes(b), lanes(c)] = block.T
            squares.append(2.0 * (block * block))

    def sum_with_gift(c):
        sum_parts(c, taken.index(c))

    last = OUTER - 1 - aside

    def add_last(where):
        add_block(last, blocks.at[last], where)

    if chunks == 4:
        end_order = [
            (add_last, slice(size, 3 * size)),
            (send_half, 1), (send_half, 2), (add_last, slice(0, size)), (add_last, slice(3 * size, width)),
            (send_parts, 1), (send_parts, 2), (last_block, 0), (send_parts, 0),
            (last_block, 3), (send_parts, 3), (sum_parts, 0), (sum_with_gift, 1), (send_strips, 0),
            (sum_with_gift, 2), (send_strips, 1), (sum_parts, 3), (send_strips, 2), (send_strips, 3),
        ]
        middle_order = [
            (add_last, slice(0, size)), (send_half, 0), (lend_halves, 0), (lend_halves, 1), (send_parts, 0),
            (add_last, slice(size, width)), (send_half, 1), (send_half, 2), (send_half, 3), (lend_parts, 0),
            (lend_parts, 1), (send_parts, 1), (send_parts, 2), (send_parts, 3), (sum_parts, 0),
            (give, 0), (give, 1), (send_strips, 0), (sum_parts, 1), (sum_parts, 2), (send_strips, 1),
            (sum_parts, 3), (send_strips, 2), (send_strips, 3),
        ]
    else:
        lots = range(len(taken))
        each = range(chunks)
        end_order = [(add_last, slice(None))] + [(send_half if c in taken else last_block, c) for c in each]
        end_order += [(send_parts, c) for c in each]
        end_order += [(sum_with_gift if c in taken else sum_parts, c) for c in each]
        end_order += [(send_strips, c) for c in each]
        middle_order = [(add_last, slice(None))]
        middle_order += [(stage, n) for stage in (lend_halves, lend_parts, give) for n in lots]
        middle_order += [(stage, c) for stage in (send_half, send_parts, sum_parts, send_strips) for c in each]

    for role, order in ((is_end, end_order), (is_middle, middle_order)):
        order += [(proj_begin, c) for c in range(chunks)]
        for c in range(chunks + 1):
            if c < chunks:
                order.append((send_gram, c))
            if c and role is is_middle:
                order.append((send_pair, c - 1))
        for c in range(chunks):
            if role is is_end:
                order.append((sum_pair, c))
            order.append((sum_gram, c))

        @pl.when(role)
        def _(order=order):
            for stage, c in order:
                stage(c)

    for step in (1, -1):
        @pl.when(both_ways(step))
        def _(step=step):
            for c in range(chunks):
                block_copy(out, step, c, True).wait_send()
    for d in range(1, OUTER):
        for step in (1, -1):
            source = out - step * d

            @pl.when(inside(source) & both_ways(step))
            def _(source=source, step=step, d=d):
                for c in range(chunks):
                    if d < OUTER - 2 or c not in taken:
                        block_copy(source, step, c).wait_send()
    for at in turn:
        for k in range(1, inner):
            piece_copy(k, at).wait_send()
    if taken:
        @pl.when(is_end)
        def _():
            for k in range(inner):
                given_copy(k).wait_send()

        @pl.when(is_middle)
        def _():
            for n in range(len(taken)):
                lent_half_copy(n).wait_send()
                for k in range(1, nchip):
                    lent_part_copy(n, k).wait_send()
                gift_copy(n).wait_send()

    @pl.when(is_middle)
    def _():
        for c in range(chunks):
            for n in range(2):
                pair_copy(c, n).wait_send()

    for c in range(chunks):
        half_copy(c).wait_send()
        for k in range(1, nchip):
            part_copy(c, k).wait_send()
        share_copy(c).wait_send()
        strip_half_copy(c).wait_send()
        for k in range(1, nchip):
            strip_part_copy(c, k).wait_send()

    for c in range(chunks + 1):
        if c < chunks:
            gram_relay(c)
        if c == chunks - 1:
            for past in range(chunks):
                proj_relay(past)
        if c:
            mirror(c - 1)

    scale = jnp.sqrt(jnp.sum(sum(squares[1:], squares[0]), keepdims=True) + 1e-06)
    root_scale = jnp.sqrt(scale)
    per_scale = 1.0 / scale
    rows = root.shape[0]

    def halves_squared(x):
        cross = dot(x[0], x[1]).astype(jnp.bfloat16)
        return dot(x[0], x[0]) + (cross.astype(jnp.float32) + cross.T.astype(jnp.float32))

    for step in range(ITERS // 2):
        w = work[0:width, :]
        w_halves = split(w)
        e = halves_squared(w_halves)
        if step == 0:
            w = w * per_scale
            e = e * (per_scale * per_scale)
        e = e - 4.5 * w
        f = 0.0625 * halves_squared(split(e)) + (0.421875 * e - 0.5390625 * w)
        f_halves = split(f)
        if step == ITERS // 2 - 1:
            rest = work[width:, :]
            got = 2.25 * rest + dot3(split(rest), f_halves)
            right[...] = got[:cols, :] * (1.0 / root_scale)
            if root.shape[1] == width:
                root[...] = got[cols:, :] * root_scale
            else:
                work[width + cols :, :] = got[cols:, :]
                long = root.shape[1]
                root[...] = work[width + cols :, pl.ds(pl.multiple_of(row * long, long), long)] * root_scale
            break
        growth = split(halves_squared(f_halves) + 4.5 * f)
        if step == 0:
            for c in range(chunks):
                proj_end(c)
            work[width : width + cols, :] = plane[pl.ds(pl.multiple_of(inn * cols, cols), cols), :]
            work[width + cols :, :] = work[pl.ds(pl.multiple_of(col * rows, rows), rows), :] * per_scale
        rest = work[width:, :]
        work[width:, :] = 2.25 * rest + dot3(split(rest), f_halves)
        for start in range(0, width, LANES):
            band, after = slice(start, start + LANES), slice(start + LANES, width)
            product = dot3([half[band] for half in w_halves], [half[:, start:] for half in growth])
            if step == 0:
                product = product * per_scale
            square = product[:, :LANES]
            work[band, band] = 5.0625 * w[band, band] + 0.5 * (square + square.T)
            if start + LANES < width:
                work[band, after] = 5.0625 * w[band, after] + product[:, LANES:]
                work[after, band] = work[band, after].T

    for c in range(chunks):
        proj_finish(c)
        gram_finish(c)


def solution(mesh):
    nrow, ncol = mesh.shape["row"], mesh.shape["col"]
    inner = ncol // OUTER
    nchip = nrow // 2 * inner

    def local(matrix, basis):
        cols, (depth, width) = matrix.shape[0], basis.shape
        tall = inner * cols
        size = width if LANES % (16 * nchip) else LANES
        chunks = width // size
        taken = tuple(range(1, chunks - 1))
        lots = max(len(taken), 1)
        vmem = pl.BlockSpec(memory_space=pltpu.VMEM)

        def array(*shape, dtype=jnp.float32):
            return pltpu.VMEM(shape, dtype)

        def pair(*shape):
            return [pltpu.SemaphoreType.DMA(shape)] * 2

        long = width // nrow
        root, right = pl.pallas_call(
            functools.partial(kernel, nrow, ncol, size, taken),
            out_shape=(
                array(width // ncol, width if long % LANES else long),
                array(cols, width),
            ),
            in_specs=[pl.BlockSpec(memory_space=pltpu.HBM)] * 2,
            out_specs=(vmem, vmem),
            scratch_shapes=[
                array(OUTER, cols, depth),
                array(depth, width),
                array(OUTER, depth, width),
                array(inner - 1, OUTER, cols, depth),
                array(OUTER + 1, tall, depth, dtype=jnp.bfloat16),
                array(OUTER + 1, tall, depth, dtype=jnp.bfloat16),
                array(tall, width),
                array(chunks, tall // 2, size),
                array(chunks, nchip - 1, tall // (2 * nchip), size),
                array(tall, width),
                array(tall // (2 * nchip), width, dtype=jnp.bfloat16),
                array(tall // (2 * nchip), width, dtype=jnp.bfloat16),
                array(chunks, size, width),
                array(chunks, size // 2, width),
                array(chunks, nchip - 1, size // (2 * nchip), width),
                array(chunks, OUTER, size // (2 * nchip), width),
                array(width, width),
                array(width + cols + width // ncol, width),
                array(inner, cols, depth),
                array(tall, lots * size),
                array(lots, tall // 2, size),
                array(lots, nchip - 1, tall // (2 * nchip), size),
                array(lots, tall // (2 * nchip), size),
                array(lots, tall // (2 * nchip), size),
                pltpu.SemaphoreType.DMA((OUTER, 2, chunks)),
                pltpu.SemaphoreType.DMA((OUTER, chunks)),
                *pair(inner - 1, OUTER),
                *pair(chunks),
                *pair(chunks, nchip - 1),
                *pair(chunks, nchip - 1),
                *pair(chunks, nchip),
                *pair(chunks, OUTER - 1),
                *pair(chunks, nchip - 1),
                *pair(chunks, nchip),
                pltpu.SemaphoreType.DMA((OUTER + 1,)),
                *pair(inner),
                *pair(lots),
                *pair(lots, nchip - 1),
                *pair(lots),
                *pair(chunks),
                *pair(chunks, nchip - 1),
            ],
            compiler_params=pltpu.CompilerParams(
                collective_id=0, has_side_effects=True, vmem_limit_bytes=VMEM
            ),
        )(matrix, basis)
        if long % LANES == 0:
            return root.T, right
        part = lax.dynamic_slice(root, (0, lax.axis_index("row") * long), (width // ncol, long))
        return part.T, right

    return jax.shard_map(
        local,
        mesh=mesh,
        in_specs=(P("col", "row"), P(("row", "col"), None)),
        out_specs=(P("row", "col"), P("col", None)),
        check_vma=False,
    )
```
